32 devices in a mesh: dp: 2 (over x), tp: 16 (over y, z, core).
Axes of the slice: x: 2, y: 2, z: 4, core: 2. Of those that a mesh axis runs over, the one named last changes fastest.
Arguments:
- x: bfloat16 [4096, 3072], P('dp'), parts along dimension 0
- dy: bfloat16 [4096, 3072], P('dp'), parts along dimension 0
- gate: bfloat16 [4096, 8192], P('dp', 'tp'), parts along dimension 0
- up: bfloat16 [4096, 8192], P('dp', 'tp'), parts along dimension 0
- w_gate: bfloat16 [3072, 8192], P(None, 'tp')
- w_up: bfloat16 [3072, 8192], P(None, 'tp')
- w_down: bfloat16 [8192, 3072], P('tp')
Outputs:
- output 1: bfloat16 [4096, 3072], P('dp'), parts along dimension 0
- output 2: bfloat16 [6144, 8192], P('dp', 'tp'), parts along dimension 0
- output 3: bfloat16 [6144, 8192], P('dp', 'tp'), parts along dimension 0
- output 4: bfloat16 [16384, 3072], P(('dp', 'tp')), parts along dimension 0
There are 2 independent parts. The reference program is written for one: setup_inputs(seed, part) draws one part's arguments, and reference() takes and returns one part's arrays. A program takes and returns all parts, laid end to end along the dimension named above; an argument that names none is the same for every part.
All inputs are finite; a program needn't handle non-finite values.
Results may differ from the reference program's by a relative error of at most 0.012.
Values are sent between devices in bfloat16 or wider.
A program may use at most 2 GiB of HBM per device.

```python
import jax
import jax.numpy as jnp

ROWS = 2048
D = 3072
FF = 8192


def act(gate, up):
    return jax.nn.silu(gate) * up


def setup_inputs(seed: int = 0, part: int = 0) -> dict:
    kx, ky, ka, kb, kg, ku, kd = jax.random.split(jax.random.key(seed), 7)
    kx, ky, ka, kb = (jax.random.fold_in(k, part) for k in (kx, ky, ka, kb))
    drawn = {
        "x": jax.random.normal(kx, (ROWS, D), jnp.float32),
        "dy": jax.random.normal(ky, (ROWS, D), jnp.float32),
        "gate": jax.random.normal(ka, (ROWS, FF), jnp.float32),
        "up": jax.random.normal(kb, (ROWS, FF), jnp.float32),
        "w_gate": jax.random.normal(kg, (D, FF), jnp.float32) * D**-0.5,
        "w_up": jax.random.normal(ku, (D, FF), jnp.float32) * D**-0.5,
        "w_down": jax.random.normal(kd, (FF, D), jnp.float32) * FF**-0.5,
    }
    return {k: v.astype(jnp.bfloat16) for k, v in drawn.items()}


def reference(x, dy, gate, up, w_gate, w_up, w_down):
    hidden, back = jax.vjp(act, gate.astype(jnp.float32), up.astype(jnp.float32))
    d_hidden = jnp.dot(dy, w_down.T, preferred_element_type=jnp.float32)
    d_gate, d_up = (g.astype(jnp.bfloat16) for g in back(d_hidden))
    dx = jnp.dot(d_gate, w_gate.T, preferred_element_type=jnp.float32) + jnp.dot(d_up, w_up.T, preferred_element_type=jnp.float32)
    dw_gate = jnp.dot(x.T, d_gate, preferred_element_type=jnp.float32)
    dw_up = jnp.dot(x.T, d_up, preferred_element_type=jnp.float32)
    dw_down = jnp.dot(hidden.astype(jnp.bfloat16).T, dy, preferred_element_type=jnp.float32)
    return tuple(g.astype(jnp.bfloat16) for g in (dx, dw_gate, dw_up, dw_down))
```

```python
import jax
import jax.numpy as jnp
from jax import lax
from jax.experimental import pallas as pl
from jax.experimental.pallas import tpu as pltpu
from jax.sharding import PartitionSpec as P

MESH = pl.DeviceIdType.MESH
F32, BF16 = jnp.float32, jnp.bfloat16

TOKENS, D, HID = 2048, 3072, 512
HALF = TOKENS // 2
CHIPS = 8
ROWS = HALF // CHIPS
Q = 4
COLS = D // Q
TILE = 256
TILES = D // TILE


def dot(a, b, contract):
    return lax.dot_general(a, b, (contract, ((), ())), preferred_element_type=F32)


def ring_kernel(
    x, dy, gate, up, w_gate, w_up, w_down,
    dx, dw_gate, dw_up, dw_down,
    wg, wu, wd, dyt, gt, ut, xt, own, stage, dgu, hid,
    w_sem, t_sem, x_sem, free,
    sib_s, sib_r, rs_s, rs_r, ag_s, ag_r, fin_s, fin_r,
):
    me = lax.axis_index("tp")
    core = lax.rem(me, 2)
    chip = me // 2
    y, z = chip // 4, lax.rem(chip, 4)
    pos = z + y * (7 - 2 * z)
    turn = 1 - 2 * core

    def device(position, c):
        p = lax.rem(position + CHIPS, CHIPS)
        back = p // 4
        zz = p + back * (7 - 2 * p)
        return (back * 4 + zz) * 2 + c

    down, upstream = device(pos + turn, core), device(pos - turn, core)
    sibling = me + turn

    for name, src, dst in ((0, w_down, wd), (1, w_gate, wg), (2, w_up, wu)):
        pltpu.make_async_copy(src, dst, w_sem.at[name]).start()

    def chunk(t, c_turn):
        return lax.rem(pos - c_turn * t + 2 * CHIPS, CHIPS)

    def mine(t):
        return pl.multiple_of(core * HALF + chunk(t, turn) * ROWS, ROWS)

    def theirs(t):
        return pl.multiple_of((1 - core) * HALF + chunk(t, -turn) * ROWS, ROWS)

    def landing(t, c):
        return pl.multiple_of((1 - c) * HALF + t * ROWS, ROWS)

    def tiles(t):
        slot = lax.rem(t, 2)
        out = []
        for k, (src, dst) in enumerate(((dy, dyt), (gate, gt), (up, ut))):
            for h, r in enumerate((mine(t), theirs(t))):
                out.append(pltpu.make_async_copy(
                    src.at[pl.ds(r, ROWS)], dst.at[slot, pl.ds(h * ROWS, ROWS)],
                    t_sem.at[slot, 2 * k + h]))
        return out

    def load(t):
        for c in tiles(t):
            c.start()

    load(0)

    barrier = pltpu.get_barrier_semaphore()
    for d in (down, upstream, sibling):
        pl.semaphore_signal(barrier, inc=1, device_id={"tp": d}, device_id_type=MESH)
    pl.semaphore_wait(barrier, 3)

    def remote(src, dst, s, r, to):
        return pltpu.make_async_remote_copy(
            src_ref=src, dst_ref=dst, send_sem=s, recv_sem=r,
            device_id={"tp": to}, device_id_type=MESH)

    def signal(k, to):
        pl.semaphore_signal(free.at[k], inc=1, device_id={"tp": to}, device_id_type=MESH)

    def cols(q):
        return pl.ds(pl.multiple_of(q * COLS, COLS), COLS)

    def sib_copy(t, q):
        return remote(stage.at[lax.rem(t, 2), :, cols(q)],
                      dx.at[pl.ds(landing(t, 1 - core), ROWS), cols(q)],
                      sib_s.at[t, q], sib_r.at[t, q], sibling)

    def sib_wait(t, q):
        return remote(stage.at[lax.rem(t, 2), :, cols(q)],
                      dx.at[pl.ds(landing(t, core), ROWS), cols(q)],
                      sib_s.at[t, q], sib_r.at[t, q], sibling)

    def rs_copy(t, q):
        at = dx.at[pl.ds(mine(t), ROWS), cols(q)]
        return remote(at, at, rs_s.at[t, q], rs_r.at[t, q], down)

    def rs_wait(t, q):
        at = dx.at[pl.ds(mine(t + 1), ROWS), cols(q)]
        return remote(at, at, rs_s.at[t, q], rs_r.at[t, q], down)

    def ag_copy(t, q):
        at = dx.at[pl.ds(mine(t + 7), ROWS), cols(q)]
        return remote(at, at, ag_s.at[t, q], ag_r.at[t, q], down)

    def ag_wait(t, q):
        at = dx.at[pl.ds(mine(t + 8), ROWS), cols(q)]
        return remote(at, at, ag_s.at[t, q], ag_r.at[t, q], down)

    def fin_copy(t, q):
        at = dx.at[pl.ds(mine(t + 7), ROWS), cols(q)]
        return remote(at, at, fin_s.at[t, q], fin_r.at[t, q], sibling)

    def fin_wait(t, q):
        at = dx.at[pl.ds(theirs(t + 7), ROWS), cols(q)]
        return remote(at, at, fin_s.at[t, q], fin_r.at[t, q], sibling)

    def hidden_part(t):
        slot = lax.rem(t, 2)
        for c in tiles(t):
            c.wait()

        @pl.when(t == 0)
        def _():
            pltpu.make_async_copy(w_down, wd, w_sem.at[0]).wait()

        dh = dot(dyt[slot], wd[...], ((1,), (1,)))
        g, u = gt[slot].astype(F32), ut[slot].astype(F32)
        sig = jax.nn.sigmoid(g)
        silu = g * sig
        d_up = (dh * silu).astype(BF16)
        d_gate = (dh * u * (sig * (1 + g * (1 - sig)))).astype(BF16)
        h = (silu * u).astype(BF16)
        for k, r in enumerate((mine(t), theirs(t))):
            at, part = pl.ds(r, ROWS), slice(k * ROWS, (k + 1) * ROWS)
            dgu[at, :HID] = d_gate[part]
            dgu[at, HID:] = d_up[part]
            hid[at] = h[part]

        @pl.when(t == 0)
        def _():
            pltpu.make_async_copy(w_gate, wg, w_sem.at[1]).wait()
            pltpu.make_async_copy(w_up, wu, w_sem.at[2]).wait()

    def term_part(t, q):
        slot = lax.rem(t, 2)
        a = jnp.concatenate([dgu[pl.ds(mine(t), ROWS)], dgu[pl.ds(theirs(t), ROWS)]], axis=0)
        v = (dot(a[:, :HID], wg[q * COLS:(q + 1) * COLS], ((1,), (1,)))
             + dot(a[:, HID:], wu[q * COLS:(q + 1) * COLS], ((1,), (1,))))

        @pl.when(t >= 2)
        def _():
            sib_copy(t - 2, q).wait_send()

        stage[slot, :, q * COLS:(q + 1) * COLS] = v[ROWS:].astype(BF16)
        sib_copy(t, q).start()
        own[slot, :, q * COLS:(q + 1) * COLS] = v[:ROWS]

    def sum_part(t, q):
        slot = lax.rem(t, 2)
        at = pl.ds(mine(t), ROWS)
        sib_wait(t, q).wait_recv()
        c = slice(q * COLS, (q + 1) * COLS)

        def local():
            return own[slot, :, c] + dx[pl.ds(landing(t, core), ROWS), c].astype(F32)

        @pl.when(t == 0)
        def _():
            dx[at, c] = local().astype(BF16)

        @pl.when(t > 0)
        def _():
            rs_wait(t - 1, q).wait_recv()
            rs_copy(t - 1, q).wait_send()
            dx[at, c] = (local() + dx[at, c].astype(F32)).astype(BF16)

        @pl.when(t < CHIPS - 1)
        def _():
            rs_copy(t, q).start()

        @pl.when(t == CHIPS - 1)
        def _():
            ag_copy(0, q).start()

    def xtile(i):
        slot = lax.rem(i, 2)
        return lambda src: pltpu.make_async_copy(
            src.at[:, pl.ds(pl.multiple_of(lax.rem(i, TILES) * TILE, TILE), TILE)],
            xt.at[slot], x_sem.at[slot])

    def load_x(i):
        @pl.when(i < TILES)
        def _():
            xtile(i)(x).start()

        @pl.when((i >= TILES) & (i < 2 * TILES))
        def _():
            xtile(i)(dy).start()

    load(1)
    hidden_part(0)
    for q in range(Q):
        term_part(0, q)

    def rs_stage(t, carry):
        @pl.when(t + 1 < CHIPS)
        def _():
            load(t + 1)

        hidden_part(t)
        for q in range(Q):
            term_part(t, q)
            sum_part(t - 1, q)
        return carry

    lax.fori_loop(1, CHIPS, rs_stage, 0)
    load_x(0)
    signal(1, upstream)
    pl.semaphore_wait(free.at[1], 1)
    for q in range(Q):
        sum_part(CHIPS - 1, q)
    signal(0, sibling)
    signal(2, upstream)
    pl.semaphore_wait(free.at[0], 1)
    for q in range(Q):
        fin_copy(0, q).start()

    def ag_step(i, carry):
        t, q = i // Q, lax.rem(i, Q)
        slot = lax.rem(i, 2)
        load_x(i + 1)

        @pl.when(i < 2 * TILES)
        def _():
            xtile(i)(x).wait()

        at = pl.ds(pl.multiple_of(lax.rem(i, TILES) * TILE, TILE), TILE)

        @pl.when(i < TILES)
        def _():
            v = dot(xt[slot], dgu[...], ((0,), (0,))).astype(BF16)
            dw_gate[at] = v[:, :HID]
            dw_up[at] = v[:, HID:]

        @pl.when((i >= TILES) & (i < 2 * TILES))
        def _():
            dw_down[:, at] = dot(hid[...], xt[slot], ((0,), (0,))).astype(BF16)

        ag_wait(t, q).wait_recv()

        @pl.when(i == (CHIPS - 3) * Q)
        def _():
            pl.semaphore_wait(free.at[2], 1)

        @pl.when(t < CHIPS - 2)
        def _():
            ag_copy(t + 1, q).start()

        fin_copy(t + 1, q).start()
        return carry

    lax.fori_loop(0, (CHIPS - 1) * Q, ag_step, 0)

    def drain(i, carry):
        t, q = i // Q, lax.rem(i, Q)

        @pl.when(t < CHIPS - 1)
        def _():
            ag_copy(t, q).wait_send()

        @pl.when(t >= CHIPS - 2)
        def _():
            sib_copy(t, q).wait_send()

        fin_copy(t, q).wait_send()
        fin_wait(t, q).wait_recv()
        return carry

    lax.fori_loop(0, CHIPS * Q, drain, 0)


def flush_kernel(*refs):
    sem = refs[-1]
    n = (len(refs) - 1) // 2
    copies = [pltpu.make_async_copy(refs[k], refs[n + k], sem.at[k]) for k in range(n)]
    for c in copies:
        c.start()
    for c in copies:
        c.wait()


def solution(mesh):
    dma = pltpu.SemaphoreType.DMA
    shapes = ((TOKENS, D), (D, HID), (D, HID), (HID, D))

    def step(x, dy, gate, up, w_gate, w_up, w_down):
        hbm = pl.BlockSpec(memory_space=pltpu.HBM)
        vmem = pl.BlockSpec(memory_space=pltpu.VMEM)
        held = pl.pallas_call(
            ring_kernel,
            out_shape=tuple(pltpu.VMEM(s, BF16) for s in shapes),
            in_specs=[hbm] * 7,
            out_specs=(vmem,) * 4,
            scratch_shapes=[
                pltpu.VMEM((D, HID), BF16), pltpu.VMEM((D, HID), BF16), pltpu.VMEM((HID, D), BF16),
                pltpu.VMEM((2, 2 * ROWS, D), BF16),
                pltpu.VMEM((2, 2 * ROWS, HID), BF16), pltpu.VMEM((2, 2 * ROWS, HID), BF16),
                pltpu.VMEM((2, TOKENS, TILE), BF16),
                pltpu.VMEM((2, ROWS, D), F32), pltpu.VMEM((2, ROWS, D), BF16),
                pltpu.VMEM((TOKENS, 2 * HID), BF16), pltpu.VMEM((TOKENS, HID), BF16),
                dma((3,)), dma((2, 6)), dma((2,)), pltpu.SemaphoreType.REGULAR((3,)),
                dma((CHIPS, Q)), dma((CHIPS, Q)),
                dma((CHIPS - 1, Q)), dma((CHIPS - 1, Q)),
                dma((CHIPS - 1, Q)), dma((CHIPS - 1, Q)),
                dma((CHIPS, Q)), dma((CHIPS, Q)),
            ],
            compiler_params=pltpu.CompilerParams(
                collective_id=0, has_side_effects=True, vmem_limit_bytes=40 * 2**20),
        )(x, dy, gate, up, w_gate, w_up, w_down)
        return pl.pallas_call(
            flush_kernel,
            out_shape=tuple(jax.ShapeDtypeStruct(s, BF16) for s in shapes),
            in_specs=[vmem] * 4,
            out_specs=(hbm,) * 4,
            scratch_shapes=[dma((4,))],
            compiler_params=pltpu.CompilerParams(vmem_limit_bytes=2 * 2**20),
        )(*held)

    tokens, columns, rows = P("dp", None), P(None, "tp"), P("tp", None)
    return jax.shard_map(
        step,
        mesh=mesh,
        in_specs=(tokens, tokens, P("dp", "tp"), P("dp", "tp"), columns, columns, rows),
        out_specs=(tokens, P("dp", "tp"), P("dp", "tp"), P(("dp", "tp"), None)),
        check_vma=False,
    )
```

```python
import jax
import jax.numpy as jnp
from jax import lax
from jax.experimental import pallas as pl
from jax.experimental.pallas import tpu as pltpu
from jax.sharding import PartitionSpec as P

MESH = pl.DeviceIdType.MESH
F32, BF16 = jnp.float32, jnp.bfloat16

TOKENS, D, HID = 2048, 3072, 512
HALF = TOKENS // 2
CHIPS = 8
ROWS = HALF // CHIPS
Q = 4
COLS = D // Q
TILE = 256
TILES = D // TILE
PARTS = 4


def dot(a, b, contract):
    return lax.dot_general(a, b, (contract, ((), ())), preferred_element_type=F32)


def ring_kernel(
    x, dy, gate, up, w_gate, w_up, w_down,
    dx, dw_gate, dw_up, dw_down,
    wg, wu, wd, dyt, gt, ut, xt, own, stage, dgu, hid,
    w_sem, t_sem, x_sem, free,
    sib_s, sib_r, rs_s, rs_r, ag_s, ag_r, fin_s, fin_r,
):
    me = lax.axis_index("tp")
    core = lax.rem(me, 2)
    chip = me // 2
    y, z = chip // 4, lax.rem(chip, 4)
    pos = z + y * (7 - 2 * z)
    turn = 1 - 2 * core

    def device(position, c):
        p = lax.rem(position + CHIPS, CHIPS)
        back = p // 4
        zz = p + back * (7 - 2 * p)
        return (back * 4 + zz) * 2 + c

    down, upstream = device(pos + turn, core), device(pos - turn, core)
    sibling = me + turn

    weights = [pltpu.make_async_copy(src, dst, w_sem.at[k])
               for k, (src, dst) in enumerate(((w_down, wd), (w_gate, wg), (w_up, wu)))]
    weights[0].start()

    def chunk(t, c_turn):
        return lax.rem(pos - c_turn * t + 2 * CHIPS, CHIPS)

    def mine(t):
        return pl.multiple_of(core * HALF + chunk(t, turn) * ROWS, ROWS)

    def theirs(t):
        return pl.multiple_of((1 - core) * HALF + chunk(t, -turn) * ROWS, ROWS)

    def landing(t, c):
        return pl.multiple_of((1 - c) * HALF + t * ROWS, ROWS)

    def tiles(t):
        slot = lax.rem(t, 2)
        out = []
        for k, (src, dst) in enumerate(((dy, dyt), (gate, gt), (up, ut))):
            for h, r in enumerate((mine(t), theirs(t))):
                out.append(pltpu.make_async_copy(
                    src.at[pl.ds(r, ROWS)], dst.at[slot, pl.ds(h * ROWS, ROWS)],
                    t_sem.at[slot, 2 * k + h]))
        return out

    def load(t):
        for c in tiles(t):
            c.start()

    load(0)
    weights[1].start()
    weights[2].start()

    barrier = pltpu.get_barrier_semaphore()
    for d in (down, upstream, sibling):
        pl.semaphore_signal(barrier, inc=1, device_id={"tp": d}, device_id_type=MESH)
    pl.semaphore_wait(barrier, 3)

    def remote(src, dst, s, r, to):
        return pltpu.make_async_remote_copy(
            src_ref=src, dst_ref=dst, send_sem=s, recv_sem=r,
            device_id={"tp": to}, device_id_type=MESH)

    def signal(k, to):
        pl.semaphore_signal(free.at[k], inc=1, device_id={"tp": to}, device_id_type=MESH)

    def cols(q):
        return pl.ds(pl.multiple_of(q * COLS, COLS), COLS)

    def sib_copy(t, q):
        return remote(stage.at[lax.rem(t, 2), :, cols(q)],
                      dx.at[pl.ds(landing(t, 1 - core), ROWS), cols(q)],
                      sib_s.at[t, q], sib_r.at[t, q], sibling)

    def sib_wait(t, q):
        return remote(stage.at[lax.rem(t, 2), :, cols(q)],
                      dx.at[pl.ds(landing(t, core), ROWS), cols(q)],
                      sib_s.at[t, q], sib_r.at[t, q], sibling)

    def rs_copy(t, q):
        at = dx.at[pl.ds(mine(t), ROWS), cols(q)]
        return remote(at, at, rs_s.at[t, q], rs_r.at[t, q], down)

    def rs_wait(t, q):
        at = dx.at[pl.ds(mine(t + 1), ROWS), cols(q)]
        return remote(at, at, rs_s.at[t, q], rs_r.at[t, q], down)

    def ag_copy(t, q):
        at = dx.at[pl.ds(mine(t + 7), ROWS), cols(q)]
        return remote(at, at, ag_s.at[t, q], ag_r.at[t, q], down)

    def ag_wait(t, q):
        at = dx.at[pl.ds(mine(t + 8), ROWS), cols(q)]
        return remote(at, at, ag_s.at[t, q], ag_r.at[t, q], down)

    def fin_copy(t, q):
        at = dx.at[pl.ds(mine(t + 7), ROWS), cols(q)]
        return remote(at, at, fin_s.at[t, q], fin_r.at[t, q], sibling)

    def fin_wait(t, q):
        at = dx.at[pl.ds(theirs(t + 7), ROWS), cols(q)]
        return remote(at, at, fin_s.at[t, q], fin_r.at[t, q], sibling)

    def hidden_part(t):
        slot = lax.rem(t, 2)
        for c in tiles(t):
            c.wait()
        dh = dot(dyt[slot], wd[...], ((1,), (1,)))
        g, u = gt[slot].astype(F32), ut[slot].astype(F32)
        sig = jax.nn.sigmoid(g)
        silu = g * sig
        d_up = (dh * silu).astype(BF16)
        d_gate = (dh * u * (sig * (1 + g * (1 - sig)))).astype(BF16)
        h = (silu * u).astype(BF16)
        for k, r in enumerate((mine(t), theirs(t))):
            at, part = pl.ds(r, ROWS), slice(k * ROWS, (k + 1) * ROWS)
            dgu[at, :HID] = d_gate[part]
            dgu[at, HID:] = d_up[part]
            hid[at] = h[part]

    def term_part(t, q):
        slot = lax.rem(t, 2)
        a = jnp.concatenate([dgu[pl.ds(mine(t), ROWS)], dgu[pl.ds(theirs(t), ROWS)]], axis=0)
        v = (dot(a[:, :HID], wg[q * COLS:(q + 1) * COLS], ((1,), (1,)))
             + dot(a[:, HID:], wu[q * COLS:(q + 1) * COLS], ((1,), (1,))))

        @pl.when(t >= 2)
        def _():
            sib_copy(t - 2, q).wait_send()

        stage[slot, :, q * COLS:(q + 1) * COLS] = v[ROWS:].astype(BF16)
        sib_copy(t, q).start()
        own[slot, :, q * COLS:(q + 1) * COLS] = v[:ROWS]

    def sum_part(t, q):
        slot = lax.rem(t, 2)
        at = pl.ds(mine(t), ROWS)
        sib_wait(t, q).wait_recv()
        c = slice(q * COLS, (q + 1) * COLS)

        def local():
            return own[slot, :, c] + dx[pl.ds(landing(t, core), ROWS), c].astype(F32)

        @pl.when(t == 0)
        def _():
            dx[at, c] = local().astype(BF16)

        @pl.when(t > 0)
        def _():
            rs_wait(t - 1, q).wait_recv()
            rs_copy(t - 1, q).wait_send()
            dx[at, c] = (local() + dx[at, c].astype(F32)).astype(BF16)

        @pl.when(t < CHIPS - 1)
        def _():
            rs_copy(t, q).start()

        @pl.when(t == CHIPS - 1)
        def _():
            ag_copy(0, q).start()

    def xtile(i):
        slot = lax.rem(i, 2)
        return lambda src: pltpu.make_async_copy(
            src.at[:, pl.ds(pl.multiple_of(lax.rem(i, TILES) * TILE, TILE), TILE)],
            xt.at[slot], x_sem.at[slot])

    def load_x(i):
        @pl.when(i < TILES)
        def _():
            xtile(i)(x).start()

        @pl.when((i >= TILES) & (i < 2 * TILES))
        def _():
            xtile(i)(dy).start()

    def rs_stage(t):
        for q in range(Q):
            term_part(t, q)
            if q:
                sum_part(t, q - 1)
        sum_part(t, Q - 1)

    def rs_body(t, carry):
        @pl.when(t + 1 < CHIPS)
        def _():
            load(t + 1)

        hidden_part(t)

        @pl.when(t == CHIPS - 1)
        def _():
            load_x(0)
            signal(1, upstream)
            pl.semaphore_wait(free.at[1], 1)

        rs_stage(t)
        return carry

    weights[0].wait()
    hidden_part(0)
    load(1)
    weights[1].wait()
    weights[2].wait()
    rs_stage(0)
    lax.fori_loop(1, CHIPS, rs_body, 0)
    signal(0, sibling)
    signal(2, upstream)
    pl.semaphore_wait(free.at[0], 1)
    for q in range(Q):
        fin_copy(0, q).start()

    def ag_step(i, carry):
        t, q = i // Q, lax.rem(i, Q)
        slot = lax.rem(i, 2)
        load_x(i + 1)

        @pl.when(i < 2 * TILES)
        def _():
            xtile(i)(x).wait()

        at = pl.ds(pl.multiple_of(lax.rem(i, TILES) * TILE, TILE), TILE)

        @pl.when(i < TILES)
        def _():
            v = dot(xt[slot], dgu[...], ((0,), (0,))).astype(BF16)
            dw_gate[at] = v[:, :HID]
            dw_up[at] = v[:, HID:]

        @pl.when((i >= TILES) & (i < 2 * TILES))
        def _():
            dw_down[:, at] = dot(hid[...], xt[slot], ((0,), (0,))).astype(BF16)

        ag_wait(t, q).wait_recv()

        @pl.when(i == (CHIPS - 3) * Q)
        def _():
            pl.semaphore_wait(free.at[2], 1)

        @pl.when(t < CHIPS - 2)
        def _():
            ag_copy(t + 1, q).start()

        fin_copy(t + 1, q).start()
        return carry

    lax.fori_loop(0, (CHIPS - 1) * Q, ag_step, 0)

    def drain(i, carry):
        t, q = i // Q, lax.rem(i, Q)

        @pl.when(t < CHIPS - 1)
        def _():
            ag_copy(t, q).wait_send()

        @pl.when(t >= CHIPS - 2)
        def _():
            sib_copy(t, q).wait_send()

        fin_copy(t, q).wait_send()
        fin_wait(t, q).wait_recv()
        return carry

    lax.fori_loop(0, CHIPS * Q, drain, 0)


def flush_kernel(*refs):
    sem = refs[-1]
    n = (len(refs) - 1) // 2
    copies = []
    for k in range(n):
        rows = refs[k].shape[0] // PARTS
        for p in range(PARTS):
            at = pl.ds(p * rows, rows)
            copies.append(pltpu.make_async_copy(refs[k].at[at], refs[n + k].at[at], sem.at[k, p]))
    for c in copies:
        c.start()
    for c in copies:
        c.wait()


def solution(mesh):
    dma = pltpu.SemaphoreType.DMA
    shapes = ((TOKENS, D), (D, HID), (D, HID), (HID, D))

    def step(x, dy, gate, up, w_gate, w_up, w_down):
        hbm = pl.BlockSpec(memory_space=pltpu.HBM)
        vmem = pl.BlockSpec(memory_space=pltpu.VMEM)
        held = pl.pallas_call(
            ring_kernel,
            out_shape=tuple(pltpu.VMEM(s, BF16) for s in shapes),
            in_specs=[hbm] * 7,
            out_specs=(vmem,) * 4,
            scratch_shapes=[
                pltpu.VMEM((D, HID), BF16), pltpu.VMEM((D, HID), BF16), pltpu.VMEM((HID, D), BF16),
                pltpu.VMEM((2, 2 * ROWS, D), BF16),
                pltpu.VMEM((2, 2 * ROWS, HID), BF16), pltpu.VMEM((2, 2 * ROWS, HID), BF16),
                pltpu.VMEM((2, TOKENS, TILE), BF16),
                pltpu.VMEM((2, ROWS, D), F32), pltpu.VMEM((2, ROWS, D), BF16),
                pltpu.VMEM((TOKENS, 2 * HID), BF16), pltpu.VMEM((TOKENS, HID), BF16),
                dma((3,)), dma((2, 6)), dma((2,)), pltpu.SemaphoreType.REGULAR((3,)),
                dma((CHIPS, Q)), dma((CHIPS, Q)),
                dma((CHIPS - 1, Q)), dma((CHIPS - 1, Q)),
                dma((CHIPS - 1, Q)), dma((CHIPS - 1, Q)),
                dma((CHIPS, Q)), dma((CHIPS, Q)),
            ],
            compiler_params=pltpu.CompilerParams(
                collective_id=0, has_side_effects=True, vmem_limit_bytes=40 * 2**20),
        )(x, dy, gate, up, w_gate, w_up, w_down)
        return pl.pallas_call(
            flush_kernel,
            out_shape=tuple(jax.ShapeDtypeStruct(s, BF16) for s in shapes),
            in_specs=[vmem] * 4,
            out_specs=(hbm,) * 4,
            scratch_shapes=[dma((4, PARTS))],
            compiler_params=pltpu.CompilerParams(vmem_limit_bytes=2 * 2**20),
        )(*held)

    tokens, columns, rows = P("dp", None), P(None, "tp"), P("tp", None)
    return jax.shard_map(
        step,
        mesh=mesh,
        in_specs=(tokens, tokens, P("dp", "tp"), P("dp", "tp"), columns, columns, rows),
        out_specs=(tokens, P("dp", "tp"), P("dp", "tp"), P(("dp", "tp"), None)),
        check_vma=False,
    )
```

```python
import jax
import jax.numpy as jnp
from jax import lax
from jax.experimental import pallas as pl
from jax.experimental.pallas import tpu as pltpu
from jax.sharding import PartitionSpec as P

MESH = pl.DeviceIdType.MESH
F32, BF16 = jnp.float32, jnp.bfloat16

TOKENS, D, HID = 2048, 3072, 512
HALF = TOKENS // 2
STAGES = 8
ROWS = HALF // STAGES
BLOCK = ROWS // 4
Q = 4
COLS = D // Q
UNITS = 2 * STAGES
WIDE = D // 2
WA = 896
WB = WIDE - WA
TILE = 256
TILES = D // TILE
PARTS = 4

END = dict(loc=2.0, lA=4.64, lB=2.47, Amo=11.33, Bse=10.53, Ams=32.77, Bse2=36.9, bAmo=43.27, fin=50)
MID = dict(loc=2.0, lA=7.27, Bo=2.1, Amo=11.74, Bs=4.3, Ams=13.66, Bsm2=6.12, bAms=33.59, bAmo=36.27,
           bBse=39.43, bBom=9.75, bBoe=45.08, fin=49.7)
LOOPS = UNITS + max(int(o) // 2 for o in (*END.values(), *MID.values()))


def dot(a, b, contract):
    return lax.dot_general(a, b, (contract, ((), ())), preferred_element_type=F32)


def tree_kernel(
    x, dy, gate, up, w_gate, w_up, w_down,
    dx, dw_gate, dw_up, dw_down,
    dyt, gt, ut, xt, loc, stage, dgu, hid, lz, lr, lx,
    w_sem, t_sem, x_sem, free,
    sib_s, sib_r, fin_s, fin_r, sA, sB, rrA, rzA, bA, rzB, rxB, rrB, bB,
):
    me = lax.axis_index("tp")
    core = lax.rem(me, 2)
    chip = me // 2
    y, z = chip // 4, lax.rem(chip, 4)
    side = z // 2
    o, n = 1 - side, 1 - y
    is_end = z * (3 - z) == 0
    is_mid = z * (3 - z) > 0
    inward = 1 - 2 * side
    sibling = me + 1 - 2 * core

    def device(yy, zz):
        return (yy * 4 + zz) * 2 + core

    rung, inner, outer = device(n, z), device(y, z + inward), device(y, z - inward)

    wg, wu, wd = dw_gate, dw_up, dw_down
    weights = [pltpu.make_async_copy(src, dst, w_sem.at[k])
               for k, (src, dst) in enumerate(((w_down, wd), (w_gate, wg), (w_up, wu)))]
    weights[0].start()

    def mine(t):
        return pl.multiple_of(core * HALF + t * ROWS, ROWS)

    def theirs(t):
        return pl.multiple_of((1 - core) * HALF + t * ROWS, ROWS)

    def tiles(t):
        slot = lax.rem(t, 2)
        out = []
        for k, (src, dst) in enumerate(((dy, dyt), (gate, gt), (up, ut))):
            for h, r in enumerate((mine(t), theirs(t))):
                out.append(pltpu.make_async_copy(
                    src.at[pl.ds(r, ROWS)], dst.at[slot, pl.ds(h * ROWS, ROWS)],
                    t_sem.at[slot, 2 * k + h]))
        return out

    def load(t):
        for c in tiles(t):
            c.start()

    load(0)
    weights[1].start()
    weights[2].start()

    barrier = pltpu.get_barrier_semaphore()

    def greet(d):
        pl.semaphore_signal(barrier, inc=1, device_id={"tp": d}, device_id_type=MESH)

    for d in (rung, inner, sibling):
        greet(d)

    @pl.when(is_mid)
    def _():
        greet(outer)
        pl.semaphore_wait(barrier, 4)

    @pl.when(is_end)
    def _():
        pl.semaphore_wait(barrier, 3)

    def remote(src, dst, s, r, to):
        return pltpu.make_async_remote_copy(
            src_ref=src, dst_ref=dst, send_sem=s, recv_sem=r,
            device_id={"tp": to}, device_id_type=MESH)

    def cols(q):
        return pl.ds(pl.multiple_of(q * COLS, COLS), COLS)

    def sib_copy(t, q):
        return remote(stage.at[lax.rem(t, 2), :, cols(q)], dx.at[pl.ds(mine(t), ROWS), cols(q)],
                      sib_s.at[t, q], sib_r.at[t, q], sibling)

    def sib_wait(t, q):
        at = dx.at[pl.ds(theirs(t), ROWS), cols(q)]
        return remote(at, at, sib_s.at[t, q], sib_r.at[t, q], sibling)

    def hidden_part(t):
        slot = lax.rem(t, 2)
        for c in tiles(t):
            c.wait()
        dh = dot(dyt[slot], wd[...], ((1,), (1,)))
        g, u = gt[slot].astype(F32), ut[slot].astype(F32)
        sig = jax.nn.sigmoid(g)
        silu = g * sig
        d_up = (dh * silu).astype(BF16)
        d_gate = (dh * u * (sig * (1 + g * (1 - sig)))).astype(BF16)
        h = (silu * u).astype(BF16)
        for k, r in enumerate((mine(t), theirs(t))):
            at, part = pl.ds(r, ROWS), slice(k * ROWS, (k + 1) * ROWS)
            dgu[at, :HID] = d_gate[part]
            dgu[at, HID:] = d_up[part]
            hid[at] = h[part]

    def term_part(t, q):
        slot = lax.rem(t, 2)
        a = jnp.concatenate([dgu[pl.ds(mine(t), ROWS)], dgu[pl.ds(theirs(t), ROWS)]], axis=0)
        v = (dot(a[:, :HID], wg[cols(q)], ((1,), (1,)))
             + dot(a[:, HID:], wu[cols(q)], ((1,), (1,))))

        @pl.when(t >= 2)
        def _():
            sib_copy(t - 2, q).wait_send()

        stage[slot, :, cols(q)] = v[ROWS:].astype(BF16)
        sib_copy(t, q).start()
        loc[pl.ds(pl.multiple_of(t * ROWS, ROWS), ROWS), cols(q)] = v[:ROWS]

    def xtile(i):
        slot = lax.rem(i, 2)
        return lambda src: pltpu.make_async_copy(
            src.at[:, pl.ds(pl.multiple_of(lax.rem(i, TILES) * TILE, TILE), TILE)],
            xt.at[slot], x_sem.at[slot])

    def load_x(i):
        @pl.when(i < TILES)
        def _():
            xtile(i)(x).start()

        @pl.when((i >= TILES) & (i < 2 * TILES))
        def _():
            xtile(i)(dy).start()

    def grad_part(i):
        slot = lax.rem(i, 2)
        load_x(i + 1)
        xtile(i)(x).wait()
        at = pl.ds(pl.multiple_of(lax.rem(i, TILES) * TILE, TILE), TILE)

        @pl.when(i < TILES)
        def _():
            v = dot(xt[slot], dgu[...], ((0,), (0,))).astype(BF16)
            dw_gate[at] = v[:, :HID]
            dw_up[at] = v[:, HID:]

        @pl.when(i >= TILES)
        def _():
            dw_down[:, at] = dot(hid[...], xt[slot], ((0,), (0,))).astype(BF16)

    def at(ref, u, k, rows, kind, base=0):
        t, h = u // 2, lax.rem(u, 2)
        r = pl.multiple_of(base + t * ROWS + k * BLOCK, BLOCK)
        c = pl.multiple_of(h * WIDE + (WA if kind == "B" else 0), 128)
        return ref.at[pl.ds(r, rows * BLOCK), pl.ds(c, WB if kind == "B" else WA)]

    A = lambda ref, u, k, rows=1: at(ref, u, k, rows, "A")
    B = lambda ref, u, k, rows=1: at(ref, u, k, rows, "B")
    DA = lambda u, k: at(dx, u, k, 1, "A", core * HALF)
    DB = lambda u, k: at(dx, u, k, 1, "B", core * HALF)
    X = lambda u: lx.at[pl.ds(pl.multiple_of(u * BLOCK, BLOCK), BLOCK)]
    val = lambda ref: ref[...].astype(F32)
    mo, ms, no, ns = y * 2 + o, y * 2 + side, n * 2 + o, n * 2 + side
    se, sm, oe, om = side * 2, side * 2 + 1, o * 2, o * 2 + 1

    def same(ref, s, r, to):
        return remote(ref, ref, s, r, to)

    def got(ref, r):
        remote(ref, ref, sib_s.at[0, 0], r, sibling).wait_recv()

    end_sends = dict(
        lA=lambda u: same(A(lr, u, n * 2, 2), sA.at[u, 0], rrA.at[u], rung),
        lB=lambda u: same(B(lz, u, o * 2, 2), sB.at[u, 0], rzB.at[u, 0], inner),
        lX=lambda u: remote(B(lz, u, sm), X(u), sB.at[u, 1], rxB.at[u], inner),
        Amo=lambda u: same(A(lz, u, mo), sA.at[u, 1], rzA.at[u, 0], inner),
        Ams=lambda u: same(DA(u, ms), sA.at[u, 2], bA.at[u, ms], inner),
        AmsR=lambda u: same(DA(u, ms), sA.at[u, 3], bA.at[u, ms], rung),
        Bse=lambda u: remote(B(lz, u, se), B(lr, u, se), sB.at[u, 2], rrB.at[u], rung),
        Bse2=lambda u: same(DB(u, se), sB.at[u, 3], bB.at[u, se], inner),
        bAmo=lambda u: same(DA(u, mo), sA.at[u, 4], bA.at[u, mo], rung),
    )
    mid_sends = dict(
        lA=lambda u: same(A(lr, u, n * 2, 2), sA.at[u, 0], rrA.at[u], rung),
        Bo=lambda u: same(B(lz, u, o * 2, 2), sB.at[u, 0], rzB.at[u, 1], inner),
        Amo=lambda u: same(A(lz, u, mo), sA.at[u, 1], rzA.at[u, 1], inner),
        BsO=lambda u: same(B(lz, u, se), sB.at[u, 1], rzB.at[u, 1], outer),
        BsR=lambda u: remote(B(lz, u, sm), B(lr, u, sm), sB.at[u, 2], rrB.at[u], rung),
        Ams=lambda u: same(A(lz, u, ms), sA.at[u, 2], rzA.at[u, 1], outer),
        Bsm2O=lambda u: same(DB(u, sm), sB.at[u, 3], bB.at[u, sm], outer),
        Bsm2I=lambda u: same(DB(u, sm), sB.at[u, 4], bB.at[u, sm], inner),
        bAmsI=lambda u: same(DA(u, ms), sA.at[u, 3], bA.at[u, ms], inner),
        bAmsR=lambda u: same(DA(u, ms), sA.at[u, 4], bA.at[u, ms], rung),
        bAmoO=lambda u: same(DA(u, mo), sA.at[u, 5], bA.at[u, mo], outer),
        bAmoR=lambda u: same(DA(u, mo), sA.at[u, 6], bA.at[u, mo], rung),
        bBse=lambda u: same(DB(u, se), sB.at[u, 5], bB.at[u, se], inner),
        bBom=lambda u: same(DB(u, om), sB.at[u, 6], bB.at[u, om], outer),
        bBoe=lambda u: same(DB(u, oe), sB.at[u, 7], bB.at[u, oe], outer),
    )

    def fin_copy(u):
        where = dx.at[pl.ds(mine(u // 2), ROWS), pl.ds(pl.multiple_of(lax.rem(u, 2) * WIDE, WIDE), WIDE)]
        return remote(where, where, fin_s.at[u], fin_r.at[u], sibling)

    def fin_wait(u):
        got(dx.at[pl.ds(theirs(u // 2), ROWS), pl.ds(pl.multiple_of(lax.rem(u, 2) * WIDE, WIDE), WIDE)],
            fin_r.at[u])

    def put(ref, v):
        ref[...] = v.astype(BF16)

    def ev_loc(u):
        t, h = u // 2, lax.rem(u, 2)
        for k in range(2):
            q = 2 * h + k
            sib_wait(t, q).wait_recv()
            r = pl.ds(pl.multiple_of(t * ROWS, ROWS), ROWS)
            loc[r, cols(q)] += dx[pl.ds(theirs(t), ROWS), cols(q)].astype(F32)
        pl.semaphore_signal(free.at[u], inc=1, device_id={"tp": sibling}, device_id_type=MESH)

    def ev_lA(sends):
        def f(u):
            put(A(lr, u, n * 2, 2), A(loc, u, n * 2, 2)[...])
            sends["lA"](u).start()
        return f

    def fin(u):
        pl.semaphore_wait(free.at[u], 1)
        fin_copy(u).start()

    def e_lB(u):
        put(B(lz, u, o * 2, 2), B(loc, u, o * 2, 2)[...])
        end_sends["lB"](u).start()
        put(B(lz, u, sm), B(loc, u, sm)[...])
        end_sends["lX"](u).start()

    def e_Amo(u):
        got(A(lr, u, y * 2, 2), rrA.at[u])
        put(A(lz, u, mo), A(loc, u, mo)[...] + val(A(lr, u, mo)))
        end_sends["Amo"](u).start()

    def e_Ams(u):
        got(A(lz, u, ms), rzA.at[u, 1])
        put(DA(u, ms), A(loc, u, ms)[...] + val(A(lr, u, ms)) + val(A(lz, u, ms)))
        end_sends["Ams"](u).start()
        end_sends["AmsR"](u).start()

    def e_Bse(u):
        got(B(lz, u, se), rzB.at[u, 1])
        put(B(lz, u, se), B(loc, u, se)[...] + val(B(lz, u, se)))
        end_sends["Bse"](u).start()

    def e_Bse2(u):
        got(B(lr, u, se), rrB.at[u])
        put(DB(u, se), val(B(lz, u, se)) + val(B(lr, u, se)))
        end_sends["Bse2"](u).start()

    def e_bAmo(u):
        got(DA(u, mo), bA.at[u, mo])
        end_sends["bAmo"](u).start()

    def e_fin(u):
        for k in (ns, no):
            got(DA(u, k), bA.at[u, k])
        for k in (sm, om, oe):
            got(DB(u, k), bB.at[u, k])
        fin(u)

    def m_Bo(u):
        got(B(lz, u, o * 2, 2), rzB.at[u, 0])
        put(B(lz, u, o * 2, 2), B(loc, u, o * 2, 2)[...] + val(B(lz, u, o * 2, 2)))
        mid_sends["Bo"](u).start()

    def m_Amo(u):
        got(A(lr, u, y * 2, 2), rrA.at[u])
        got(A(lz, u, mo), rzA.at[u, 0])
        put(A(lz, u, mo), A(loc, u, mo)[...] + val(A(lr, u, mo)) + val(A(lz, u, mo)))
        mid_sends["Amo"](u).start()

    def m_Bs(u):
        got(B(lz, u, side * 2, 2), rzB.at[u, 1])
        put(B(lz, u, se), B(loc, u, se)[...] + val(B(lz, u, se)))
        mid_sends["BsO"](u).start()
        got(X(u), rxB.at[u])
        put(B(lz, u, sm), B(loc, u, sm)[...] + val(B(lz, u, sm)) + val(X(u)))
        mid_sends["BsR"](u).start()

    def m_Ams(u):
        got(A(lz, u, ms), rzA.at[u, 1])
        put(A(lz, u, ms), A(loc, u, ms)[...] + val(A(lr, u, ms)) + val(A(lz, u, ms)))
        mid_sends["Ams"](u).start()

    def m_Bsm2(u):
        got(B(lr, u, sm), rrB.at[u])
        put(DB(u, sm), val(B(lz, u, sm)) + val(B(lr, u, sm)))
        mid_sends["Bsm2O"](u).start()
        mid_sends["Bsm2I"](u).start()

    def m_back(where, sem, k, names):
        def f(u):
            got(where(u, k), sem.at[u, k])
            for name in names:
                mid_sends[name](u).start()
        return f

    def m_fin(u):
        for k in (ns, no):
            got(DA(u, k), bA.at[u, k])
        fin(u)

    end_events = dict(loc=ev_loc, lA=ev_lA(end_sends), lB=e_lB, Amo=e_Amo, Ams=e_Ams, Bse=e_Bse,
                      Bse2=e_Bse2, bAmo=e_bAmo, fin=e_fin)
    mid_events = dict(loc=ev_loc, lA=ev_lA(mid_sends), Bo=m_Bo, Amo=m_Amo, Bs=m_Bs, Ams=m_Ams, Bsm2=m_Bsm2,
                      bAms=m_back(DA, bA, ms, ("bAmsI", "bAmsR")), bAmo=m_back(DA, bA, mo, ("bAmoO", "bAmoR")),
                      bBse=m_back(DB, bB, se, ("bBse",)), bBom=m_back(DB, bB, om, ("bBom",)),
                      bBoe=m_back(DB, bB, oe, ("bBoe",)), fin=m_fin)

    def events(i, pos):
        for here, when, handlers in ((is_end, END, end_events), (is_mid, MID, mid_events)):
            @pl.when(here)
            def _():
                for name, off in sorted(when.items(), key=lambda kv: kv[1]):
                    if int(off) % 2 == pos:
                        u = i - int(off) // 2

                        @pl.when((u >= 0) & (u < UNITS))
                        def _():
                            handlers[name](u)

    def body(i, carry):
        t, h = i // 2, lax.rem(i, 2)

        @pl.when((i < UNITS) & (h == 0))
        def _():
            @pl.when(t + 1 < STAGES)
            def _():
                load(t + 1)

            hidden_part(t)

            @pl.when(t == 0)
            def _():
                weights[1].wait()
                weights[2].wait()

        for pos in range(2):
            @pl.when(i < UNITS)
            def _():
                term_part(t, 2 * h + pos)

            if pos == 1:
                @pl.when(i == UNITS - 1)
                def _():
                    load_x(0)

            @pl.when((i >= UNITS) & (i < UNITS + TILES))
            def _():
                grad_part(2 * (i - UNITS) + pos)

            events(i, pos)
        return carry

    weights[0].wait()
    lax.fori_loop(0, LOOPS, body, 0)

    def drain(u, carry):
        @pl.when(is_end)
        def _():
            for send in end_sends.values():
                send(u).wait_send()

        @pl.when(is_mid)
        def _():
            for send in mid_sends.values():
                send(u).wait_send()

        fin_copy(u).wait_send()
        fin_wait(u)
        return carry

    lax.fori_loop(0, UNITS, drain, 0)
    for t in (STAGES - 2, STAGES - 1):
        for q in range(Q):
            sib_copy(t, q).wait_send()


def flush_kernel(*refs):
    sem = refs[-1]
    n = (len(refs) - 1) // 2
    copies = []
    for k in range(n):
        rows = refs[k].shape[0] // PARTS
        for p in range(PARTS):
            at = pl.ds(p * rows, rows)
            copies.append(pltpu.make_async_copy(refs[k].at[at], refs[n + k].at[at], sem.at[k, p]))
    for c in copies:
        c.start()
    for c in copies:
        c.wait()


def solution(mesh):
    dma = pltpu.SemaphoreType.DMA
    shapes = ((TOKENS, D), (D, HID), (D, HID), (HID, D))

    def step(x, dy, gate, up, w_gate, w_up, w_down):
        hbm = pl.BlockSpec(memory_space=pltpu.HBM)
        vmem = pl.BlockSpec(memory_space=pltpu.VMEM)
        held = pl.pallas_call(
            tree_kernel,
            out_shape=tuple(pltpu.VMEM(s, BF16) for s in shapes),
            in_specs=[hbm] * 7,
            out_specs=(vmem,) * 4,
            scratch_shapes=[
                pltpu.VMEM((2, 2 * ROWS, D), BF16),
                pltpu.VMEM((2, 2 * ROWS, HID), BF16), pltpu.VMEM((2, 2 * ROWS, HID), BF16),
                pltpu.VMEM((2, TOKENS, TILE), BF16),
                pltpu.VMEM((HALF, D), F32), pltpu.VMEM((2, ROWS, D), BF16),
                pltpu.VMEM((TOKENS, 2 * HID), BF16), pltpu.VMEM((TOKENS, HID), BF16),
                pltpu.VMEM((HALF, D), BF16), pltpu.VMEM((HALF, D), BF16),
                pltpu.VMEM((UNITS * BLOCK, WB), BF16),
                dma((3,)), dma((2, 6)), dma((2,)), pltpu.SemaphoreType.REGULAR((UNITS,)),
                dma((STAGES, Q)), dma((STAGES, Q)), dma((UNITS,)), dma((UNITS,)),
                dma((UNITS, 7)), dma((UNITS, 8)), dma((UNITS,)), dma((UNITS, 2)), dma((UNITS, 4)),
                dma((UNITS, 2)), dma((UNITS,)), dma((UNITS,)), dma((UNITS, 4)),
            ],
            compiler_params=pltpu.CompilerParams(
                collective_id=0, has_side_effects=True, vmem_limit_bytes=42 * 2**20),
        )(x, dy, gate, up, w_gate, w_up, w_down)
        return pl.pallas_call(
            flush_kernel,
            out_shape=tuple(jax.ShapeDtypeStruct(s, BF16) for s in shapes),
            in_specs=[vmem] * 4,
            out_specs=(hbm,) * 4,
            scratch_shapes=[dma((4, PARTS))],
            compiler_params=pltpu.CompilerParams(vmem_limit_bytes=2 * 2**20),
        )(*held)

    tokens, columns, rows = P("dp", None), P(None, "tp"), P("tp", None)
    return jax.shard_map(
        step,
        mesh=mesh,
        in_specs=(tokens, tokens, P("dp", "tp"), P("dp", "tp"), columns, columns, rows),
        out_specs=(tokens, P("dp", "tp"), P("dp", "tp"), P(("dp", "tp"), None)),
        check_vma=False,
    )
```

```python
import jax
import jax.numpy as jnp
from jax import lax
from jax.experimental import pallas as pl
from jax.experimental.pallas import tpu as pltpu
from jax.sharding import PartitionSpec as P

MESH = pl.DeviceIdType.MESH
F32, BF16 = jnp.float32, jnp.bfloat16

TOKENS, D, HID = 2048, 3072, 512
HALF = TOKENS // 2
STAGES = 8
ROWS = HALF // STAGES
BLOCK = ROWS // 4
Q = 4
COLS = D // Q
UNITS = 2 * STAGES
WIDE = D // 2
WA = 1024
WB = WIDE - WA
TILE = 256
TILES = D // TILE
PARTS = 4

END = dict(loc=2.0, lA=2.1, lB=2.14, Amo=5.08, Bse=12.06, Ams=27.23, Bse2=33.68, bAmo=40.55, fin=52)
MID = dict(loc=2.0, lA=5.51, Bo=7.82, Amo=10.23, Bs=10.22, Ams=12.07, Bsm2=12.39, bAms=32.1, bAmo=35.22,
           bBse=39.16, bBom=14.54, bBoe=43.96, fin=48.63)
LOOPS = UNITS + max(int(o) // 2 for o in (*END.values(), *MID.values()))


def dot(a, b, contract):
    return lax.dot_general(a, b, (contract, ((), ())), preferred_element_type=F32)


def tree_kernel(
    x, dy, gate, up, w_gate, w_up, w_down,
    dx, dw_gate, dw_up, dw_down,
    dyt, gt, ut, xt, loc, stage, dgu, hid, lz, lr, lx,
    w_sem, t_sem, x_sem, free,
    sib_s, sib_r, fin_s, fin_r, sA, sB, rrA, rzA, bA, rzB, rxB, rrB, bB,
):
    me = lax.axis_index("tp")
    core = lax.rem(me, 2)
    chip = me // 2
    y, z = chip // 4, lax.rem(chip, 4)
    side = z // 2
    o, n = 1 - side, 1 - y
    is_end = z * (3 - z) == 0
    is_mid = z * (3 - z) > 0
    inward = 1 - 2 * side
    sibling = me + 1 - 2 * core

    def device(yy, zz):
        return (yy * 4 + zz) * 2 + core

    rung, inner, outer = device(n, z), device(y, z + inward), device(y, z - inward)

    wg, wu, wd = dw_gate, dw_up, dw_down
    weights = [pltpu.make_async_copy(src, dst, w_sem.at[k])
               for k, (src, dst) in enumerate(((w_down, wd), (w_gate, wg), (w_up, wu)))]
    weights[0].start()

    def mine(t):
        return pl.multiple_of(core * HALF + t * ROWS, ROWS)

    def theirs(t):
        return pl.multiple_of((1 - core) * HALF + t * ROWS, ROWS)

    def tiles(t):
        slot = lax.rem(t, 2)
        out = []
        for k, (src, dst) in enumerate(((dy, dyt), (gate, gt), (up, ut))):
            for h, r in enumerate((mine(t), theirs(t))):
                out.append(pltpu.make_async_copy(
                    src.at[pl.ds(r, ROWS)], dst.at[slot, pl.ds(h * ROWS, ROWS)],
                    t_sem.at[slot, 2 * k + h]))
        return out

    def load(t):
        for c in tiles(t):
            c.start()

    load(0)
    weights[1].start()
    weights[2].start()

    barrier = pltpu.get_barrier_semaphore()

    def greet(d):
        pl.semaphore_signal(barrier, inc=1, device_id={"tp": d}, device_id_type=MESH)

    for d in (rung, inner, sibling):
        greet(d)

    @pl.when(is_mid)
    def _():
        greet(outer)
        pl.semaphore_wait(barrier, 4)

    @pl.when(is_end)
    def _():
        pl.semaphore_wait(barrier, 3)

    def remote(src, dst, s, r, to):
        return pltpu.make_async_remote_copy(
            src_ref=src, dst_ref=dst, send_sem=s, recv_sem=r,
            device_id={"tp": to}, device_id_type=MESH)

    def cols(q):
        return pl.ds(pl.multiple_of(q * COLS, COLS), COLS)

    def sib_copy(t, q):
        return remote(stage.at[lax.rem(t, 2), :, cols(q)], dx.at[pl.ds(mine(t), ROWS), cols(q)],
                      sib_s.at[t, q], sib_r.at[t, q], sibling)

    def sib_wait(t, q):
        at = dx.at[pl.ds(theirs(t), ROWS), cols(q)]
        return remote(at, at, sib_s.at[t, q], sib_r.at[t, q], sibling)

    def hidden_part(t):
        slot = lax.rem(t, 2)
        for c in tiles(t):
            c.wait()
        dh = dot(dyt[slot], wd[...], ((1,), (1,)))
        g, u = gt[slot].astype(F32), ut[slot].astype(F32)
        sig = jax.nn.sigmoid(g)
        silu = g * sig
        d_up = (dh * silu).astype(BF16)
        d_gate = (dh * u * (sig * (1 + g * (1 - sig)))).astype(BF16)
        h = (silu * u).astype(BF16)
        for k, r in enumerate((mine(t), theirs(t))):
            at, part = pl.ds(r, ROWS), slice(k * ROWS, (k + 1) * ROWS)
            dgu[at, :HID] = d_gate[part]
            dgu[at, HID:] = d_up[part]
            hid[at] = h[part]

    def term_part(t, q):
        slot = lax.rem(t, 2)
        a = jnp.concatenate([dgu[pl.ds(mine(t), ROWS)], dgu[pl.ds(theirs(t), ROWS)]], axis=0)
        v = (dot(a[:, :HID], wg[cols(q)], ((1,), (1,)))
             + dot(a[:, HID:], wu[cols(q)], ((1,), (1,))))

        @pl.when(t >= 2)
        def _():
            sib_copy(t - 2, q).wait_send()

        stage[slot, :, cols(q)] = v[ROWS:].astype(BF16)
        sib_copy(t, q).start()
        loc[pl.ds(pl.multiple_of(t * ROWS, ROWS), ROWS), cols(q)] = v[:ROWS]

    def xtile(i):
        slot = lax.rem(i, 2)
        return lambda src: pltpu.make_async_copy(
            src.at[:, pl.ds(pl.multiple_of(lax.rem(i, TILES) * TILE, TILE), TILE)],
            xt.at[slot], x_sem.at[slot])

    def load_x(i):
        @pl.when(i < TILES)
        def _():
            xtile(i)(x).start()

        @pl.when((i >= TILES) & (i < 2 * TILES))
        def _():
            xtile(i)(dy).start()

    def grad_part(i):
        slot = lax.rem(i, 2)
        load_x(i + 1)
        xtile(i)(x).wait()
        at = pl.ds(pl.multiple_of(lax.rem(i, TILES) * TILE, TILE), TILE)

        @pl.when(i < TILES)
        def _():
            v = dot(xt[slot], dgu[...], ((0,), (0,))).astype(BF16)
            dw_gate[at] = v[:, :HID]
            dw_up[at] = v[:, HID:]

        @pl.when(i >= TILES)
        def _():
            dw_down[:, at] = dot(hid[...], xt[slot], ((0,), (0,))).astype(BF16)

    def at(ref, u, k, rows, kind, base=0):
        t, h = u // 2, lax.rem(u, 2)
        r = pl.multiple_of(base + t * ROWS + k * BLOCK, BLOCK)
        c = pl.multiple_of(h * WIDE + (WA if kind == "B" else 0), 128)
        return ref.at[pl.ds(r, rows * BLOCK), pl.ds(c, WB if kind == "B" else WA)]

    A = lambda ref, u, k, rows=1: at(ref, u, k, rows, "A")
    B = lambda ref, u, k, rows=1: at(ref, u, k, rows, "B")
    DA = lambda u, k: at(dx, u, k, 1, "A", core * HALF)
    DB = lambda u, k: at(dx, u, k, 1, "B", core * HALF)
    X = lambda u: lx.at[pl.ds(pl.multiple_of(u * BLOCK, BLOCK), BLOCK)]
    val = lambda ref: ref[...].astype(F32)
    mo, ms, no, ns = y * 2 + o, y * 2 + side, n * 2 + o, n * 2 + side
    se, sm, oe, om = side * 2, side * 2 + 1, o * 2, o * 2 + 1

    def same(ref, s, r, to):
        return remote(ref, ref, s, r, to)

    def got(ref, r):
        remote(ref, ref, sib_s.at[0, 0], r, sibling).wait_recv()

    end_sends = dict(
        lA=lambda u: same(A(lr, u, n * 2, 2), sA.at[u, 0], rrA.at[u], rung),
        lB=lambda u: same(B(lz, u, o * 2, 2), sB.at[u, 0], rzB.at[u, 0], inner),
        lX=lambda u: remote(B(lz, u, sm), X(u), sB.at[u, 1], rxB.at[u], inner),
        Amo=lambda u: same(A(lz, u, mo), sA.at[u, 1], rzA.at[u, 0], inner),
        Ams=lambda u: same(DA(u, ms), sA.at[u, 2], bA.at[u, ms], inner),
        AmsR=lambda u: same(DA(u, ms), sA.at[u, 3], bA.at[u, ms], rung),
        Bse=lambda u: remote(B(lz, u, se), B(lr, u, se), sB.at[u, 2], rrB.at[u], rung),
        Bse2=lambda u: same(DB(u, se), sB.at[u, 3], bB.at[u, se], inner),
        bAmo=lambda u: same(DA(u, mo), sA.at[u, 4], bA.at[u, mo], rung),
    )
    mid_sends = dict(
        lA=lambda u: same(A(lr, u, n * 2, 2), sA.at[u, 0], rrA.at[u], rung),
        Bo=lambda u: same(B(lz, u, o * 2, 2), sB.at[u, 0], rzB.at[u, 1], inner),
        Amo=lambda u: same(A(lz, u, mo), sA.at[u, 1], rzA.at[u, 1], inner),
        BsO=lambda u: same(B(lz, u, se), sB.at[u, 1], rzB.at[u, 1], outer),
        BsR=lambda u: remote(B(lz, u, sm), B(lr, u, sm), sB.at[u, 2], rrB.at[u], rung),
        Ams=lambda u: same(A(lz, u, ms), sA.at[u, 2], rzA.at[u, 1], outer),
        Bsm2O=lambda u: same(DB(u, sm), sB.at[u, 3], bB.at[u, sm], outer),
        Bsm2I=lambda u: same(DB(u, sm), sB.at[u, 4], bB.at[u, sm], inner),
        bAmsI=lambda u: same(DA(u, ms), sA.at[u, 3], bA.at[u, ms], inner),
        bAmsR=lambda u: same(DA(u, ms), sA.at[u, 4], bA.at[u, ms], rung),
        bAmoO=lambda u: same(DA(u, mo), sA.at[u, 5], bA.at[u, mo], outer),
        bAmoR=lambda u: same(DA(u, mo), sA.at[u, 6], bA.at[u, mo], rung),
        bBse=lambda u: same(DB(u, se), sB.at[u, 5], bB.at[u, se], inner),
        bBom=lambda u: same(DB(u, om), sB.at[u, 6], bB.at[u, om], outer),
        bBoe=lambda u: same(DB(u, oe), sB.at[u, 7], bB.at[u, oe], outer),
    )

    def fin_copy(u):
        where = dx.at[pl.ds(mine(u // 2), ROWS), pl.ds(pl.multiple_of(lax.rem(u, 2) * WIDE, WIDE), WIDE)]
        return remote(where, where, fin_s.at[u], fin_r.at[u], sibling)

    def fin_wait(u):
        got(dx.at[pl.ds(theirs(u // 2), ROWS), pl.ds(pl.multiple_of(lax.rem(u, 2) * WIDE, WIDE), WIDE)],
            fin_r.at[u])

    def put(ref, v):
        ref[...] = v.astype(BF16)

    def ev_loc(u):
        t, h = u // 2, lax.rem(u, 2)
        for k in range(2):
            q = 2 * h + k
            sib_wait(t, q).wait_recv()
            r = pl.ds(pl.multiple_of(t * ROWS, ROWS), ROWS)
            loc[r, cols(q)] += dx[pl.ds(theirs(t), ROWS), cols(q)].astype(F32)
        pl.semaphore_signal(free.at[u], inc=1, device_id={"tp": sibling}, device_id_type=MESH)

    def ev_lA(sends):
        def f(u):
            put(A(lr, u, n * 2, 2), A(loc, u, n * 2, 2)[...])
            sends["lA"](u).start()
        return f

    def fin(u):
        pl.semaphore_wait(free.at[u], 1)
        fin_copy(u).start()

    def e_lB(u):
        put(B(lz, u, o * 2, 2), B(loc, u, o * 2, 2)[...])
        end_sends["lB"](u).start()
        put(B(lz, u, sm), B(loc, u, sm)[...])
        end_sends["lX"](u).start()

    def e_Amo(u):
        got(A(lr, u, y * 2, 2), rrA.at[u])
        put(A(lz, u, mo), A(loc, u, mo)[...] + val(A(lr, u, mo)))
        end_sends["Amo"](u).start()

    def e_Ams(u):
        got(A(lz, u, ms), rzA.at[u, 1])
        put(DA(u, ms), A(loc, u, ms)[...] + val(A(lr, u, ms)) + val(A(lz, u, ms)))
        end_sends["Ams"](u).start()
        end_sends["AmsR"](u).start()

    def e_Bse(u):
        got(B(lz, u, se), rzB.at[u, 1])
        put(B(lz, u, se), B(loc, u, se)[...] + val(B(lz, u, se)))
        end_sends["Bse"](u).start()

    def e_Bse2(u):
        got(B(lr, u, se), rrB.at[u])
        put(DB(u, se), val(B(lz, u, se)) + val(B(lr, u, se)))
        end_sends["Bse2"](u).start()

    def e_bAmo(u):
        got(DA(u, mo), bA.at[u, mo])
        end_sends["bAmo"](u).start()

    def e_fin(u):
        for k in (ns, no):
            got(DA(u, k), bA.at[u, k])
        for k in (sm, om, oe):
            got(DB(u, k), bB.at[u, k])
        fin(u)

    def m_Bo(u):
        got(B(lz, u, o * 2, 2), rzB.at[u, 0])
        put(B(lz, u, o * 2, 2), B(loc, u, o * 2, 2)[...] + val(B(lz, u, o * 2, 2)))
        mid_sends["Bo"](u).start()

    def m_Amo(u):
        got(A(lr, u, y * 2, 2), rrA.at[u])
        got(A(lz, u, mo), rzA.at[u, 0])
        put(A(lz, u, mo), A(loc, u, mo)[...] + val(A(lr, u, mo)) + val(A(lz, u, mo)))
        mid_sends["Amo"](u).start()

    def m_Bs(u):
        got(B(lz, u, side * 2, 2), rzB.at[u, 1])
        put(B(lz, u, se), B(loc, u, se)[...] + val(B(lz, u, se)))
        mid_sends["BsO"](u).start()
        got(X(u), rxB.at[u])
        put(B(lz, u, sm), B(loc, u, sm)[...] + val(B(lz, u, sm)) + val(X(u)))
        mid_sends["BsR"](u).start()

    def m_Ams(u):
        got(A(lz, u, ms), rzA.at[u, 1])
        put(A(lz, u, ms), A(loc, u, ms)[...] + val(A(lr, u, ms)) + val(A(lz, u, ms)))
        mid_sends["Ams"](u).start()

    def m_Bsm2(u):
        got(B(lr, u, sm), rrB.at[u])
        put(DB(u, sm), val(B(lz, u, sm)) + val(B(lr, u, sm)))
        mid_sends["Bsm2O"](u).start()
        mid_sends["Bsm2I"](u).start()

    def m_back(where, sem, k, names):
        def f(u):
            got(where(u, k), sem.at[u, k])
            for name in names:
                mid_sends[name](u).start()
        return f

    def m_fin(u):
        for k in (ns, no):
            got(DA(u, k), bA.at[u, k])
        fin(u)

    end_events = dict(loc=ev_loc, lA=ev_lA(end_sends), lB=e_lB, Amo=e_Amo, Ams=e_Ams, Bse=e_Bse,
                      Bse2=e_Bse2, bAmo=e_bAmo, fin=e_fin)
    mid_events = dict(loc=ev_loc, lA=ev_lA(mid_sends), Bo=m_Bo, Amo=m_Amo, Bs=m_Bs, Ams=m_Ams, Bsm2=m_Bsm2,
                      bAms=m_back(DA, bA, ms, ("bAmsI", "bAmsR")), bAmo=m_back(DA, bA, mo, ("bAmoO", "bAmoR")),
                      bBse=m_back(DB, bB, se, ("bBse",)), bBom=m_back(DB, bB, om, ("bBom",)),
                      bBoe=m_back(DB, bB, oe, ("bBoe",)), fin=m_fin)

    def events(i, pos):
        for here, when, handlers in ((is_end, END, end_events), (is_mid, MID, mid_events)):
            @pl.when(here)
            def _():
                for name, off in sorted(when.items(), key=lambda kv: kv[1]):
                    if int(off) % 2 == pos:
                        u = i - int(off) // 2

                        @pl.when((u >= 0) & (u < UNITS))
                        def _():
                            handlers[name](u)

    def body(i, carry):
        t, h = i // 2, lax.rem(i, 2)

        @pl.when((i < UNITS) & (h == 0))
        def _():
            @pl.when(t + 1 < STAGES)
            def _():
                load(t + 1)

            hidden_part(t)

            @pl.when(t == 0)
            def _():
                weights[1].wait()
                weights[2].wait()

        for pos in range(2):
            @pl.when(i < UNITS)
            def _():
                term_part(t, 2 * h + pos)

            if pos == 1:
                @pl.when(i == UNITS - 1)
                def _():
                    load_x(0)

            @pl.when((i >= UNITS) & (i < UNITS + TILES))
            def _():
                grad_part(2 * (i - UNITS) + pos)

            events(i, pos)
        return carry

    weights[0].wait()
    lax.fori_loop(0, LOOPS, body, 0)

    def drain(u, carry):
        @pl.when(is_end)
        def _():
            for send in end_sends.values():
                send(u).wait_send()

        @pl.when(is_mid)
        def _():
            for send in mid_sends.values():
                send(u).wait_send()

        fin_copy(u).wait_send()
        fin_wait(u)
        return carry

    lax.fori_loop(0, UNITS, drain, 0)
    for t in (STAGES - 2, STAGES - 1):
        for q in range(Q):
            sib_copy(t, q).wait_send()


def flush_kernel(*refs):
    sem = refs[-1]
    n = (len(refs) - 1) // 2
    copies = []
    for k in range(n):
        rows = refs[k].shape[0] // PARTS
        for p in range(PARTS):
            at = pl.ds(p * rows, rows)
            copies.append(pltpu.make_async_copy(refs[k].at[at], refs[n + k].at[at], sem.at[k, p]))
    for c in copies:
        c.start()
    for c in copies:
        c.wait()


def solution(mesh):
    dma = pltpu.SemaphoreType.DMA
    shapes = ((TOKENS, D), (D, HID), (D, HID), (HID, D))

    def step(x, dy, gate, up, w_gate, w_up, w_down):
        hbm = pl.BlockSpec(memory_space=pltpu.HBM)
        vmem = pl.BlockSpec(memory_space=pltpu.VMEM)
        held = pl.pallas_call(
            tree_kernel,
            out_shape=tuple(pltpu.VMEM(s, BF16) for s in shapes),
            in_specs=[hbm] * 7,
            out_specs=(vmem,) * 4,
            scratch_shapes=[
                pltpu.VMEM((2, 2 * ROWS, D), BF16),
                pltpu.VMEM((2, 2 * ROWS, HID), BF16), pltpu.VMEM((2, 2 * ROWS, HID), BF16),
                pltpu.VMEM((2, TOKENS, TILE), BF16),
                pltpu.VMEM((HALF, D), F32), pltpu.VMEM((2, ROWS, D), BF16),
                pltpu.VMEM((TOKENS, 2 * HID), BF16), pltpu.VMEM((TOKENS, HID), BF16),
                pltpu.VMEM((HALF, D), BF16), pltpu.VMEM((HALF, D), BF16),
                pltpu.VMEM((UNITS * BLOCK, WB), BF16),
                dma((3,)), dma((2, 6)), dma((2,)), pltpu.SemaphoreType.REGULAR((UNITS,)),
                dma((STAGES, Q)), dma((STAGES, Q)), dma((UNITS,)), dma((UNITS,)),
                dma((UNITS, 7)), dma((UNITS, 8)), dma((UNITS,)), dma((UNITS, 2)), dma((UNITS, 4)),
                dma((UNITS, 2)), dma((UNITS,)), dma((UNITS,)), dma((UNITS, 4)),
            ],
            compiler_params=pltpu.CompilerParams(
                collective_id=0, has_side_effects=True, vmem_limit_bytes=42 * 2**20),
        )(x, dy, gate, up, w_gate, w_up, w_down)
        return pl.pallas_call(
            flush_kernel,
            out_shape=tuple(jax.ShapeDtypeStruct(s, BF16) for s in shapes),
            in_specs=[vmem] * 4,
            out_specs=(hbm,) * 4,
            scratch_shapes=[dma((4, PARTS))],
            compiler_params=pltpu.CompilerParams(vmem_limit_bytes=2 * 2**20),
        )(*held)

    tokens, columns, rows = P("dp", None), P(None, "tp"), P("tp", None)
    return jax.shard_map(
        step,
        mesh=mesh,
        in_specs=(tokens, tokens, P("dp", "tp"), P("dp", "tp"), columns, columns, rows),
        out_specs=(tokens, P("dp", "tp"), P("dp", "tp"), P(("dp", "tp"), None)),
        check_vma=False,
    )
```

```python
import jax
import jax.numpy as jnp
from jax import lax
from jax.experimental import pallas as pl
from jax.experimental.pallas import tpu as pltpu
from jax.sharding import PartitionSpec as P

MESH = pl.DeviceIdType.MESH
F32, BF16 = jnp.float32, jnp.bfloat16

TOKENS, D, HID = 2048, 3072, 512
HALF = TOKENS // 2
STAGES = 8
ROWS = HALF // STAGES
BLOCK = ROWS // 4
Q = 4
COLS = D // Q
UNITS = 2 * STAGES
WIDE = D // 2
WA = 1024
WB = WIDE - WA
TILE = 256
TILES = D // TILE
PARTS = 4

END = dict(loc=2.0, lA=3.73, lB=2.1, Amo=7.77, Bse=31.21, Ams=26.7, Bse2=34.23, bAmo=45.84, fin=56)
MID = dict(loc=2.0, lA=3.9, Bo=4.2, Amo=9.93, Bs=6.44, Ams=12.45, Bsm2=9.38, bAms=28.53,
           bAmo=31.94, fin=50.25, bBse=38.19, bBom=11.13, bBoe=44.03)
LOOPS = UNITS + max(int(o) // 2 for o in (*END.values(), *MID.values()))


def dot(a, b, contract):
    return lax.dot_general(a, b, (contract, ((), ())), preferred_element_type=F32)


def tree_kernel(
    x, dy, gate, up, w_gate, w_up, w_down,
    dx, dw_gate, dw_up, dw_down,
    dyt, gt, ut, xt, loc, stage, dgu, hid, lz, lr, lx,
    w_sem, t_sem, x_sem, free,
    sib_s, sib_r, fin_s, fin_r, sA, sB, rrA, rzA, bA, rzB, rxB, rrB, bB,
):
    me = lax.axis_index("tp")
    core = lax.rem(me, 2)
    chip = me // 2
    y, z = chip // 4, lax.rem(chip, 4)
    side = z // 2
    o, n = 1 - side, 1 - y
    is_end = z * (3 - z) == 0
    is_mid = z * (3 - z) > 0
    inward = 1 - 2 * side
    sibling = me + 1 - 2 * core

    def device(yy, zz):
        return (yy * 4 + zz) * 2 + core

    rung, inner, outer = device(n, z), device(y, z + inward), device(y, z - inward)

    wg, wu, wd = dw_gate, dw_up, dw_down
    weights = [pltpu.make_async_copy(src, dst, w_sem.at[k])
               for k, (src, dst) in enumerate(((w_down, wd), (w_gate, wg), (w_up, wu)))]
    weights[0].start()

    def mine(t):
        return pl.multiple_of(core * HALF + t * ROWS, ROWS)

    def theirs(t):
        return pl.multiple_of((1 - core) * HALF + t * ROWS, ROWS)

    def tiles(t):
        slot = lax.rem(t, 2)
        out = []
        for k, (src, dst) in enumerate(((dy, dyt), (gate, gt), (up, ut))):
            for h, r in enumerate((mine(t), theirs(t))):
                out.append(pltpu.make_async_copy(
                    src.at[pl.ds(r, ROWS)], dst.at[slot, pl.ds(h * ROWS, ROWS)],
                    t_sem.at[slot, 2 * k + h]))
        return out

    def load(t):
        for c in tiles(t):
            c.start()

    load(0)
    weights[1].start()
    weights[2].start()

    barrier = pltpu.get_barrier_semaphore()

    def greet(d):
        pl.semaphore_signal(barrier, inc=1, device_id={"tp": d}, device_id_type=MESH)

    for d in (rung, inner, sibling):
        greet(d)

    @pl.when(is_mid)
    def _():
        greet(outer)
        pl.semaphore_wait(barrier, 4)

    @pl.when(is_end)
    def _():
        pl.semaphore_wait(barrier, 3)

    def remote(src, dst, s, r, to):
        return pltpu.make_async_remote_copy(
            src_ref=src, dst_ref=dst, send_sem=s, recv_sem=r,
            device_id={"tp": to}, device_id_type=MESH)

    def cols(q):
        return pl.ds(pl.multiple_of(q * COLS, COLS), COLS)

    def sib_copy(t, q):
        return remote(stage.at[lax.rem(t, 2), :, cols(q)], dx.at[pl.ds(mine(t), ROWS), cols(q)],
                      sib_s.at[t, q], sib_r.at[t, q], sibling)

    def sib_wait(t, q):
        at = dx.at[pl.ds(theirs(t), ROWS), cols(q)]
        return remote(at, at, sib_s.at[t, q], sib_r.at[t, q], sibling)

    def hidden_part(t):
        slot = lax.rem(t, 2)
        for c in tiles(t):
            c.wait()
        dh = dot(dyt[slot], wd[...], ((1,), (1,)))
        g, u = gt[slot].astype(F32), ut[slot].astype(F32)
        sig = jax.nn.sigmoid(g)
        silu = g * sig
        d_up = (dh * silu).astype(BF16)
        d_gate = (dh * u * (sig * (1 + g * (1 - sig)))).astype(BF16)
        h = (silu * u).astype(BF16)
        for k, r in enumerate((mine(t), theirs(t))):
            at, part = pl.ds(r, ROWS), slice(k * ROWS, (k + 1) * ROWS)
            dgu[at, :HID] = d_gate[part]
            dgu[at, HID:] = d_up[part]
            hid[at] = h[part]

    def term_part(t, q):
        slot = lax.rem(t, 2)
        a = jnp.concatenate([dgu[pl.ds(mine(t), ROWS)], dgu[pl.ds(theirs(t), ROWS)]], axis=0)
        v = (dot(a[:, :HID], wg[cols(q)], ((1,), (1,)))
             + dot(a[:, HID:], wu[cols(q)], ((1,), (1,))))

        @pl.when(t >= 2)
        def _():
            sib_copy(t - 2, q).wait_send()

        stage[slot, :, cols(q)] = v[ROWS:].astype(BF16)
        sib_copy(t, q).start()
        loc[pl.ds(pl.multiple_of(t * ROWS, ROWS), ROWS), cols(q)] = v[:ROWS]

    def xtile(i):
        slot = lax.rem(i, 2)
        return lambda src: pltpu.make_async_copy(
            src.at[:, pl.ds(pl.multiple_of(lax.rem(i, TILES) * TILE, TILE), TILE)],
            xt.at[slot], x_sem.at[slot])

    def load_x(i):
        @pl.when(i < TILES)
        def _():
            xtile(i)(x).start()

        @pl.when((i >= TILES) & (i < 2 * TILES))
        def _():
            xtile(i)(dy).start()

    def grad_part(i):
        slot = lax.rem(i, 2)
        load_x(i + 1)
        xtile(i)(x).wait()
        at = pl.ds(pl.multiple_of(lax.rem(i, TILES) * TILE, TILE), TILE)

        @pl.when(i < TILES)
        def _():
            v = dot(xt[slot], dgu[...], ((0,), (0,))).astype(BF16)
            dw_gate[at] = v[:, :HID]
            dw_up[at] = v[:, HID:]

        @pl.when(i >= TILES)
        def _():
            dw_down[:, at] = dot(hid[...], xt[slot], ((0,), (0,))).astype(BF16)

    def at(ref, u, k, rows, kind, base=0):
        t, h = u // 2, lax.rem(u, 2)
        r = pl.multiple_of(base + t * ROWS + k * BLOCK, BLOCK)
        c = pl.multiple_of(h * WIDE + (WA if kind == "B" else 0), 128)
        return ref.at[pl.ds(r, rows * BLOCK), pl.ds(c, WB if kind == "B" else WA)]

    A = lambda ref, u, k, rows=1: at(ref, u, k, rows, "A")
    B = lambda ref, u, k, rows=1: at(ref, u, k, rows, "B")
    DA = lambda u, k: at(dx, u, k, 1, "A", core * HALF)
    DB = lambda u, k: at(dx, u, k, 1, "B", core * HALF)
    X = lambda u: lx.at[pl.ds(pl.multiple_of(u * BLOCK, BLOCK), BLOCK)]
    val = lambda ref: ref[...].astype(F32)
    mo, ms, no, ns = y * 2 + o, y * 2 + side, n * 2 + o, n * 2 + side
    se, sm, oe, om = side * 2, side * 2 + 1, o * 2, o * 2 + 1

    def same(ref, s, r, to):
        return remote(ref, ref, s, r, to)

    def got(ref, r):
        remote(ref, ref, sib_s.at[0, 0], r, sibling).wait_recv()

    end_sends = dict(
        lA=lambda u: same(A(lr, u, n * 2, 2), sA.at[u, 0], rrA.at[u], rung),
        lB=lambda u: same(B(lz, u, o * 2, 2), sB.at[u, 0], rzB.at[u, 0], inner),
        lX=lambda u: remote(B(lz, u, sm), X(u), sB.at[u, 1], rxB.at[u], inner),
        Amo=lambda u: same(A(lz, u, mo), sA.at[u, 1], rzA.at[u, 0], inner),
        Ams=lambda u: same(DA(u, ms), sA.at[u, 2], bA.at[u, ms], inner),
        AmsR=lambda u: same(DA(u, ms), sA.at[u, 3], bA.at[u, ms], rung),
        Bse=lambda u: remote(B(lz, u, se), B(lr, u, se), sB.at[u, 2], rrB.at[u], rung),
        Bse2=lambda u: same(DB(u, se), sB.at[u, 3], bB.at[u, se], inner),
        bAmo=lambda u: same(DA(u, mo), sA.at[u, 4], bA.at[u, mo], rung),
    )
    mid_sends = dict(
        lA=lambda u: same(A(lr, u, n * 2, 2), sA.at[u, 0], rrA.at[u], rung),
        Bo=lambda u: same(B(lz, u, o * 2, 2), sB.at[u, 0], rzB.at[u, 1], inner),
        Amo=lambda u: same(A(lz, u, mo), sA.at[u, 1], rzA.at[u, 1], inner),
        BsO=lambda u: same(B(lz, u, se), sB.at[u, 1], rzB.at[u, 1], outer),
        BsR=lambda u: remote(B(lz, u, sm), B(lr, u, sm), sB.at[u, 2], rrB.at[u], rung),
        Ams=lambda u: same(A(lz, u, ms), sA.at[u, 2], rzA.at[u, 1], outer),
        Bsm2O=lambda u: same(DB(u, sm), sB.at[u, 3], bB.at[u, sm], outer),
        Bsm2I=lambda u: same(DB(u, sm), sB.at[u, 4], bB.at[u, sm], inner),
        bAmsI=lambda u: same(DA(u, ms), sA.at[u, 3], bA.at[u, ms], inner),
        bAmsR=lambda u: same(DA(u, ms), sA.at[u, 4], bA.at[u, ms], rung),
        bAmoO=lambda u: same(DA(u, mo), sA.at[u, 5], bA.at[u, mo], outer),
        bAmoR=lambda u: same(DA(u, mo), sA.at[u, 6], bA.at[u, mo], rung),
        bBse=lambda u: same(DB(u, se), sB.at[u, 5], bB.at[u, se], inner),
        bBom=lambda u: same(DB(u, om), sB.at[u, 6], bB.at[u, om], outer),
        bBoe=lambda u: same(DB(u, oe), sB.at[u, 7], bB.at[u, oe], outer),
    )

    def fin_copy(u):
        where = dx.at[pl.ds(mine(u // 2), ROWS), pl.ds(pl.multiple_of(lax.rem(u, 2) * WIDE, WIDE), WIDE)]
        return remote(where, where, fin_s.at[u], fin_r.at[u], sibling)

    def fin_wait(u):
        got(dx.at[pl.ds(theirs(u // 2), ROWS), pl.ds(pl.multiple_of(lax.rem(u, 2) * WIDE, WIDE), WIDE)],
            fin_r.at[u])

    def put(ref, v):
        ref[...] = v.astype(BF16)

    def ev_loc(u):
        t, h = u // 2, lax.rem(u, 2)
        for k in range(2):
            q = 2 * h + k
            sib_wait(t, q).wait_recv()
            r = pl.ds(pl.multiple_of(t * ROWS, ROWS), ROWS)
            loc[r, cols(q)] += dx[pl.ds(theirs(t), ROWS), cols(q)].astype(F32)
        pl.semaphore_signal(free.at[u], inc=1, device_id={"tp": sibling}, device_id_type=MESH)

    def ev_lA(sends):
        def f(u):
            put(A(lr, u, n * 2, 2), A(loc, u, n * 2, 2)[...])
            sends["lA"](u).start()
        return f

    def fin(u):
        pl.semaphore_wait(free.at[u], 1)
        fin_copy(u).start()

    def e_lB(u):
        put(B(lz, u, o * 2, 2), B(loc, u, o * 2, 2)[...])
        end_sends["lB"](u).start()
        put(B(lz, u, sm), B(loc, u, sm)[...])
        end_sends["lX"](u).start()

    def e_Amo(u):
        got(A(lr, u, y * 2, 2), rrA.at[u])
        put(A(lz, u, mo), A(loc, u, mo)[...] + val(A(lr, u, mo)))
        end_sends["Amo"](u).start()

    def e_Ams(u):
        got(A(lz, u, ms), rzA.at[u, 1])
        put(DA(u, ms), A(loc, u, ms)[...] + val(A(lr, u, ms)) + val(A(lz, u, ms)))
        end_sends["Ams"](u).start()
        end_sends["AmsR"](u).start()

    def e_Bse(u):
        got(B(lz, u, se), rzB.at[u, 1])
        put(B(lz, u, se), B(loc, u, se)[...] + val(B(lz, u, se)))
        end_sends["Bse"](u).start()

    def e_Bse2(u):
        got(B(lr, u, se), rrB.at[u])
        put(DB(u, se), val(B(lz, u, se)) + val(B(lr, u, se)))
        end_sends["Bse2"](u).start()

    def e_bAmo(u):
        got(DA(u, mo), bA.at[u, mo])
        end_sends["bAmo"](u).start()

    def e_fin(u):
        for k in (ns, no):
            got(DA(u, k), bA.at[u, k])
        for k in (sm, om, oe):
            got(DB(u, k), bB.at[u, k])
        fin(u)

    def m_Bo(u):
        got(B(lz, u, o * 2, 2), rzB.at[u, 0])
        put(B(lz, u, o * 2, 2), B(loc, u, o * 2, 2)[...] + val(B(lz, u, o * 2, 2)))
        mid_sends["Bo"](u).start()

    def m_Amo(u):
        got(A(lr, u, y * 2, 2), rrA.at[u])
        got(A(lz, u, mo), rzA.at[u, 0])
        put(A(lz, u, mo), A(loc, u, mo)[...] + val(A(lr, u, mo)) + val(A(lz, u, mo)))
        mid_sends["Amo"](u).start()

    def m_Bs(u):
        got(B(lz, u, side * 2, 2), rzB.at[u, 1])
        put(B(lz, u, se), B(loc, u, se)[...] + val(B(lz, u, se)))
        mid_sends["BsO"](u).start()
        got(X(u), rxB.at[u])
        put(B(lz, u, sm), B(loc, u, sm)[...] + val(B(lz, u, sm)) + val(X(u)))
        mid_sends["BsR"](u).start()

    def m_Ams(u):
        got(A(lz, u, ms), rzA.at[u, 1])
        put(A(lz, u, ms), A(loc, u, ms)[...] + val(A(lr, u, ms)) + val(A(lz, u, ms)))
        mid_sends["Ams"](u).start()

    def m_Bsm2(u):
        got(B(lr, u, sm), rrB.at[u])
        put(DB(u, sm), val(B(lz, u, sm)) + val(B(lr, u, sm)))
        mid_sends["Bsm2O"](u).start()
        mid_sends["Bsm2I"](u).start()

    def m_back(where, sem, k, names):
        def f(u):
            got(where(u, k), sem.at[u, k])
            for name in names:
                mid_sends[name](u).start()
        return f

    def m_fin(u):
        for k in (ns, no):
            got(DA(u, k), bA.at[u, k])
        fin(u)

    end_events = dict(loc=ev_loc, lA=ev_lA(end_sends), lB=e_lB, Amo=e_Amo, Ams=e_Ams, Bse=e_Bse,
                      Bse2=e_Bse2, bAmo=e_bAmo, fin=e_fin)
    mid_events = dict(loc=ev_loc, lA=ev_lA(mid_sends), Bo=m_Bo, Amo=m_Amo, Bs=m_Bs, Ams=m_Ams, Bsm2=m_Bsm2,
                      bAms=m_back(DA, bA, ms, ("bAmsI", "bAmsR")), bAmo=m_back(DA, bA, mo, ("bAmoO", "bAmoR")),
                      bBse=m_back(DB, bB, se, ("bBse",)), bBom=m_back(DB, bB, om, ("bBom",)),
                      bBoe=m_back(DB, bB, oe, ("bBoe",)), fin=m_fin)

    def events(i, pos):
        for here, when, handlers in ((is_end, END, end_events), (is_mid, MID, mid_events)):
            @pl.when(here)
            def _():
                for name, off in sorted(when.items(), key=lambda kv: kv[1]):
                    if int(off) % 2 == pos:
                        u = i - int(off) // 2

                        @pl.when((u >= 0) & (u < UNITS))
                        def _():
                            handlers[name](u)

    def body(i, carry):
        t, h = i // 2, lax.rem(i, 2)

        @pl.when((i < UNITS) & (h == 0))
        def _():
            @pl.when(t + 1 < STAGES)
            def _():
                load(t + 1)

            hidden_part(t)

            @pl.when(t == 0)
            def _():
                weights[1].wait()
                weights[2].wait()

        for pos in range(2):
            @pl.when(i < UNITS)
            def _():
                term_part(t, 2 * h + pos)

            if pos == 1:
                @pl.when(i == UNITS - 1)
                def _():
                    load_x(0)

            @pl.when((i >= UNITS) & (i < UNITS + TILES))
            def _():
                grad_part(2 * (i - UNITS) + pos)

            events(i, pos)
        return carry

    weights[0].wait()
    lax.fori_loop(0, LOOPS, body, 0)

    def drain(u, carry):
        @pl.when(is_end)
        def _():
            for send in end_sends.values():
                send(u).wait_send()

        @pl.when(is_mid)
        def _():
            for send in mid_sends.values():
                send(u).wait_send()

        fin_copy(u).wait_send()
        fin_wait(u)
        return carry

    lax.fori_loop(0, UNITS, drain, 0)
    for t in (STAGES - 2, STAGES - 1):
        for q in range(Q):
            sib_copy(t, q).wait_send()


def flush_kernel(*refs):
    sem = refs[-1]
    n = (len(refs) - 1) // 2
    copies = []
    for k in range(n):
        rows = refs[k].shape[0] // PARTS
        for p in range(PARTS):
            at = pl.ds(p * rows, rows)
            copies.append(pltpu.make_async_copy(refs[k].at[at], refs[n + k].at[at], sem.at[k, p]))
    for c in copies:
        c.start()
    for c in copies:
        c.wait()


def solution(mesh):
    dma = pltpu.SemaphoreType.DMA
    shapes = ((TOKENS, D), (D, HID), (D, HID), (HID, D))

    def step(x, dy, gate, up, w_gate, w_up, w_down):
        hbm = pl.BlockSpec(memory_space=pltpu.HBM)
        vmem = pl.BlockSpec(memory_space=pltpu.VMEM)
        held = pl.pallas_call(
            tree_kernel,
            out_shape=tuple(pltpu.VMEM(s, BF16) for s in shapes),
            in_specs=[hbm] * 7,
            out_specs=(vmem,) * 4,
            scratch_shapes=[
                pltpu.VMEM((2, 2 * ROWS, D), BF16),
                pltpu.VMEM((2, 2 * ROWS, HID), BF16), pltpu.VMEM((2, 2 * ROWS, HID), BF16),
                pltpu.VMEM((2, TOKENS, TILE), BF16),
                pltpu.VMEM((HALF, D), F32), pltpu.VMEM((2, ROWS, D), BF16),
                pltpu.VMEM((TOKENS, 2 * HID), BF16), pltpu.VMEM((TOKENS, HID), BF16),
                pltpu.VMEM((HALF, D), BF16), pltpu.VMEM((HALF, D), BF16),
                pltpu.VMEM((UNITS * BLOCK, WB), BF16),
                dma((3,)), dma((2, 6)), dma((2,)), pltpu.SemaphoreType.REGULAR((UNITS,)),
                dma((STAGES, Q)), dma((STAGES, Q)), dma((UNITS,)), dma((UNITS,)),
                dma((UNITS, 7)), dma((UNITS, 8)), dma((UNITS,)), dma((UNITS, 2)), dma((UNITS, 4)),
                dma((UNITS, 2)), dma((UNITS,)), dma((UNITS,)), dma((UNITS, 4)),
            ],
            compiler_params=pltpu.CompilerParams(
                collective_id=0, has_side_effects=True, vmem_limit_bytes=42 * 2**20),
        )(x, dy, gate, up, w_gate, w_up, w_down)
        return pl.pallas_call(
            flush_kernel,
            out_shape=tuple(jax.ShapeDtypeStruct(s, BF16) for s in shapes),
            in_specs=[vmem] * 4,
            out_specs=(hbm,) * 4,
            scratch_shapes=[dma((4, PARTS))],
            compiler_params=pltpu.CompilerParams(vmem_limit_bytes=2 * 2**20),
        )(*held)

    tokens, columns, rows = P("dp", None), P(None, "tp"), P("tp", None)
    return jax.shard_map(
        step,
        mesh=mesh,
        in_specs=(tokens, tokens, P("dp", "tp"), P("dp", "tp"), columns, columns, rows),
        out_specs=(tokens, P("dp", "tp"), P("dp", "tp"), P(("dp", "tp"), None)),
        check_vma=False,
    )
```

```python
import jax
import jax.numpy as jnp
from jax import lax
from jax.experimental import pallas as pl
from jax.experimental.pallas import tpu as pltpu
from jax.sharding import PartitionSpec as P

MESH = pl.DeviceIdType.MESH
F32, BF16 = jnp.float32, jnp.bfloat16

TOKENS, D, HID = 2048, 3072, 512
HALF = TOKENS // 2
STAGES = 8
ROWS = HALF // STAGES
BLOCK = ROWS // 4
Q = 4
COLS = D // Q
UNITS = 2 * STAGES
WIDE = D // 2
WA = 1024
WB = WIDE - WA
TILE = 256
TILES = D // TILE
PARTS = 4

END = dict(loc=2.0, lA=3.73, lB=2.1, Amo=7.77, Bse=31.21, Ams=26.7, Bse2=34.23, bAmo=45.84, fin=56)
MID = dict(loc=2.0, lA=3.9, Bo=4.2, Amo=9.93, Bs=6.44, Ams=12.45, Bsm2=9.38, bAms=28.53,
           bAmo=31.94, fin=50.25, bBse=38.19, bBom=11.13, bBoe=44.03)
LOOPS = UNITS + max(int(o) // 2 for o in (*END.values(), *MID.values()))


def dot(a, b, contract):
    return lax.dot_general(a, b, (contract, ((), ())), preferred_element_type=F32)


def tree_kernel(
    x, dy, gate, up, w_gate, w_up, w_down,
    dx, dw_gate, dw_up, dw_down,
    dyt, gt, ut, xt, loc, stage, dgu, hid, lz, lr, lx,
    w_sem, t_sem, x_sem, free,
    sib_s, sib_r, fin_s, fin_r, sA, sB, rrA, rzA, bA, rzB, rxB, rrB, bB,
):
    me = lax.axis_index("tp")
    core = lax.rem(me, 2)
    chip = me // 2
    y, z = chip // 4, lax.rem(chip, 4)
    side = z // 2
    o, n = 1 - side, 1 - y
    is_end = z * (3 - z) == 0
    is_mid = z * (3 - z) > 0
    inward = 1 - 2 * side
    sibling = me + 1 - 2 * core

    def device(yy, zz):
        return (yy * 4 + zz) * 2 + core

    rung, inner, outer = device(n, z), device(y, z + inward), device(y, z - inward)

    wg, wu, wd = dw_gate, dw_up, dw_down
    weights = [pltpu.make_async_copy(src, dst, w_sem.at[k])
               for k, (src, dst) in enumerate(((w_down, wd), (w_gate, wg), (w_up, wu)))]
    weights[0].start()

    def mine(t):
        return pl.multiple_of(core * HALF + t * ROWS, ROWS)

    def theirs(t):
        return pl.multiple_of((1 - core) * HALF + t * ROWS, ROWS)

    def tiles(t):
        slot = lax.rem(t, 2)
        out = []
        for k, (src, dst) in enumerate(((dy, dyt), (gate, gt), (up, ut))):
            for h, r in enumerate((mine(t), theirs(t))):
                out.append(pltpu.make_async_copy(
                    src.at[pl.ds(r, ROWS)], dst.at[slot, pl.ds(h * ROWS, ROWS)],
                    t_sem.at[slot, 2 * k + h]))
        return out

    def load(t):
        for c in tiles(t):
            c.start()

    load(0)
    weights[1].start()
    weights[2].start()

    barrier = pltpu.get_barrier_semaphore()

    def greet(d):
        pl.semaphore_signal(barrier, inc=1, device_id={"tp": d}, device_id_type=MESH)

    for d in (rung, inner, sibling):
        greet(d)

    @pl.when(is_mid)
    def _():
        greet(outer)
        pl.semaphore_wait(barrier, 4)

    @pl.when(is_end)
    def _():
        pl.semaphore_wait(barrier, 3)

    def remote(src, dst, s, r, to):
        return pltpu.make_async_remote_copy(
            src_ref=src, dst_ref=dst, send_sem=s, recv_sem=r,
            device_id={"tp": to}, device_id_type=MESH)

    def cols(q):
        return pl.ds(pl.multiple_of(q * COLS, COLS), COLS)

    def sib_copy(t, q):
        return remote(stage.at[lax.rem(t, 2), :, cols(q)], dx.at[pl.ds(mine(t), ROWS), cols(q)],
                      sib_s.at[t, q], sib_r.at[t, q], sibling)

    def sib_wait(t, q):
        at = dx.at[pl.ds(theirs(t), ROWS), cols(q)]
        return remote(at, at, sib_s.at[t, q], sib_r.at[t, q], sibling)

    def hidden_part(t):
        slot = lax.rem(t, 2)
        for c in tiles(t):
            c.wait()
        dh = dot(dyt[slot], wd[...], ((1,), (1,)))
        g, u = gt[slot].astype(F32), ut[slot].astype(F32)
        sig = jax.nn.sigmoid(g)
        silu = g * sig
        d_up = (dh * silu).astype(BF16)
        d_gate = (dh * u * (sig * (1 + g * (1 - sig)))).astype(BF16)
        h = (silu * u).astype(BF16)
        for k, r in enumerate((mine(t), theirs(t))):
            at, part = pl.ds(r, ROWS), slice(k * ROWS, (k + 1) * ROWS)
            dgu[at, :HID] = d_gate[part]
            dgu[at, HID:] = d_up[part]
            hid[at] = h[part]

    def term_part(t, q):
        slot = lax.rem(t, 2)
        a = jnp.concatenate([dgu[pl.ds(mine(t), ROWS)], dgu[pl.ds(theirs(t), ROWS)]], axis=0)
        v = (dot(a[:, :HID], wg[cols(q)], ((1,), (1,)))
             + dot(a[:, HID:], wu[cols(q)], ((1,), (1,))))

        @pl.when(t >= 2)
        def _():
            sib_copy(t - 2, q).wait_send()

        stage[slot, :, cols(q)] = v[ROWS:].astype(BF16)
        sib_copy(t, q).start()
        loc[pl.ds(pl.multiple_of(t * ROWS, ROWS), ROWS), cols(q)] = v[:ROWS]

    def xtile(i):
        slot = lax.rem(i, 2)
        return lambda src: pltpu.make_async_copy(
            src.at[:, pl.ds(pl.multiple_of(lax.rem(i, TILES) * TILE, TILE), TILE)],
            xt.at[slot], x_sem.at[slot])

    def load_x(i):
        @pl.when(i < TILES)
        def _():
            xtile(i)(x).start()

        @pl.when((i >= TILES) & (i < 2 * TILES))
        def _():
            xtile(i)(dy).start()

    def grad_part(i):
        slot = lax.rem(i, 2)
        load_x(i + 1)
        xtile(i)(x).wait()
        at = pl.ds(pl.multiple_of(lax.rem(i, TILES) * TILE, TILE), TILE)

        @pl.when(i < TILES)
        def _():
            v = dot(xt[slot], dgu[...], ((0,), (0,))).astype(BF16)
            dw_gate[at] = v[:, :HID]
            dw_up[at] = v[:, HID:]

        @pl.when(i >= TILES)
        def _():
            dw_down[:, at] = dot(hid[...], xt[slot], ((0,), (0,))).astype(BF16)

    def at(ref, u, k, rows, kind, base=0):
        t, h = u // 2, lax.rem(u, 2)
        r = pl.multiple_of(base + t * ROWS + k * BLOCK, BLOCK)
        c = pl.multiple_of(h * WIDE + (WA if kind == "B" else 0), 128)
        return ref.at[pl.ds(r, rows * BLOCK), pl.ds(c, WB if kind == "B" else WA)]

    A = lambda ref, u, k, rows=1: at(ref, u, k, rows, "A")
    B = lambda ref, u, k, rows=1: at(ref, u, k, rows, "B")
    DA = lambda u, k: at(dx, u, k, 1, "A", core * HALF)
    DB = lambda u, k: at(dx, u, k, 1, "B", core * HALF)
    X = lambda u: lx.at[pl.ds(pl.multiple_of(u * BLOCK, BLOCK), BLOCK)]
    val = lambda ref: ref[...].astype(F32)
    mo, ms, no, ns = y * 2 + o, y * 2 + side, n * 2 + o, n * 2 + side
    se, sm, oe, om = side * 2, side * 2 + 1, o * 2, o * 2 + 1

    def same(ref, s, r, to):
        return remote(ref, ref, s, r, to)

    def got(ref, r):
        remote(ref, ref, sib_s.at[0, 0], r, sibling).wait_recv()

    end_sends = dict(
        lA=lambda u: same(A(lr, u, n * 2, 2), sA.at[u, 0], rrA.at[u], rung),
        lB=lambda u: same(B(lz, u, o * 2, 2), sB.at[u, 0], rzB.at[u, 0], inner),
        lX=lambda u: remote(B(lz, u, sm), X(u), sB.at[u, 1], rxB.at[u], inner),
        Amo=lambda u: same(A(lz, u, mo), sA.at[u, 1], rzA.at[u, 0], inner),
        Ams=lambda u: same(DA(u, ms), sA.at[u, 2], bA.at[u, ms], inner),
        AmsR=lambda u: same(DA(u, ms), sA.at[u, 3], bA.at[u, ms], rung),
        Bse=lambda u: remote(B(lz, u, se), B(lr, u, se), sB.at[u, 2], rrB.at[u], rung),
        Bse2=lambda u: same(DB(u, se), sB.at[u, 3], bB.at[u, se], inner),
        bAmo=lambda u: same(DA(u, mo), sA.at[u, 4], bA.at[u, mo], rung),
    )
    mid_sends = dict(
        lA=lambda u: same(A(lr, u, n * 2, 2), sA.at[u, 0], rrA.at[u], rung),
        Bo=lambda u: same(B(lz, u, o * 2, 2), sB.at[u, 0], rzB.at[u, 1], inner),
        Amo=lambda u: same(A(lz, u, mo), sA.at[u, 1], rzA.at[u, 1], inner),
        BsO=lambda u: same(B(lz, u, se), sB.at[u, 1], rzB.at[u, 1], outer),
        BsR=lambda u: remote(B(lz, u, sm), B(lr, u, sm), sB.at[u, 2], rrB.at[u], rung),
        Ams=lambda u: same(A(lz, u, ms), sA.at[u, 2], rzA.at[u, 1], outer),
        Bsm2O=lambda u: same(DB(u, sm), sB.at[u, 3], bB.at[u, sm], outer),
        Bsm2I=lambda u: same(DB(u, sm), sB.at[u, 4], bB.at[u, sm], inner),
        bAmsI=lambda u: same(DA(u, ms), sA.at[u, 3], bA.at[u, ms], inner),
        bAmsR=lambda u: same(DA(u, ms), sA.at[u, 4], bA.at[u, ms], rung),
        bAmoO=lambda u: same(DA(u, mo), sA.at[u, 5], bA.at[u, mo], outer),
        bAmoR=lambda u: same(DA(u, mo), sA.at[u, 6], bA.at[u, mo], rung),
        bBse=lambda u: same(DB(u, se), sB.at[u, 5], bB.at[u, se], inner),
        bBom=lambda u: same(DB(u, om), sB.at[u, 6], bB.at[u, om], outer),
        bBoe=lambda u: same(DB(u, oe), sB.at[u, 7], bB.at[u, oe], outer),
    )

    def fin_at(u, k, row):
        c = pl.multiple_of(lax.rem(u, 2) * WIDE + k * WA, 128)
        return dx.at[pl.ds(row(u // 2), ROWS), pl.ds(c, (WA, WB)[k])]

    def fin_copy(u, k):
        where = fin_at(u, k, mine)
        return remote(where, where, fin_s.at[u, k], fin_r.at[u, k], sibling)

    def fin_wait(u, k):
        got(fin_at(u, k, theirs), fin_r.at[u, k])

    def put(ref, v):
        ref[...] = v.astype(BF16)

    def ev_loc(u):
        t, h = u // 2, lax.rem(u, 2)
        for k in range(2):
            q = 2 * h + k
            sib_wait(t, q).wait_recv()
            r = pl.ds(pl.multiple_of(t * ROWS, ROWS), ROWS)
            loc[r, cols(q)] += dx[pl.ds(theirs(t), ROWS), cols(q)].astype(F32)
        pl.semaphore_signal(free.at[u], inc=1, device_id={"tp": sibling}, device_id_type=MESH)

    def ev_lA(sends):
        def f(u):
            put(A(lr, u, n * 2, 2), A(loc, u, n * 2, 2)[...])
            sends["lA"](u).start()
        return f

    def e_lB(u):
        put(B(lz, u, o * 2, 2), B(loc, u, o * 2, 2)[...])
        end_sends["lB"](u).start()
        put(B(lz, u, sm), B(loc, u, sm)[...])
        end_sends["lX"](u).start()

    def e_Amo(u):
        got(A(lr, u, y * 2, 2), rrA.at[u])
        put(A(lz, u, mo), A(loc, u, mo)[...] + val(A(lr, u, mo)))
        end_sends["Amo"](u).start()

    def e_Ams(u):
        got(A(lz, u, ms), rzA.at[u, 1])
        put(DA(u, ms), A(loc, u, ms)[...] + val(A(lr, u, ms)) + val(A(lz, u, ms)))
        end_sends["Ams"](u).start()
        end_sends["AmsR"](u).start()

    def e_Bse(u):
        got(B(lz, u, se), rzB.at[u, 1])
        put(B(lz, u, se), B(loc, u, se)[...] + val(B(lz, u, se)))
        end_sends["Bse"](u).start()

    def e_Bse2(u):
        got(B(lr, u, se), rrB.at[u])
        put(DB(u, se), val(B(lz, u, se)) + val(B(lr, u, se)))
        end_sends["Bse2"](u).start()

    def e_bAmo(u):
        got(DA(u, mo), bA.at[u, mo])
        end_sends["bAmo"](u).start()

    def e_fin(u):
        pl.semaphore_wait(free.at[u], 1)
        for k in (sm, om, oe):
            got(DB(u, k), bB.at[u, k])
        fin_copy(u, 1).start()
        for k in (ns, no):
            got(DA(u, k), bA.at[u, k])
        fin_copy(u, 0).start()

    def m_Bo(u):
        got(B(lz, u, o * 2, 2), rzB.at[u, 0])
        put(B(lz, u, o * 2, 2), B(loc, u, o * 2, 2)[...] + val(B(lz, u, o * 2, 2)))
        mid_sends["Bo"](u).start()

    def m_Amo(u):
        got(A(lr, u, y * 2, 2), rrA.at[u])
        got(A(lz, u, mo), rzA.at[u, 0])
        put(A(lz, u, mo), A(loc, u, mo)[...] + val(A(lr, u, mo)) + val(A(lz, u, mo)))
        mid_sends["Amo"](u).start()

    def m_Bs(u):
        got(B(lz, u, side * 2, 2), rzB.at[u, 1])
        put(B(lz, u, se), B(loc, u, se)[...] + val(B(lz, u, se)))
        mid_sends["BsO"](u).start()
        got(X(u), rxB.at[u])
        put(B(lz, u, sm), B(loc, u, sm)[...] + val(B(lz, u, sm)) + val(X(u)))
        mid_sends["BsR"](u).start()

    def m_Ams(u):
        got(A(lz, u, ms), rzA.at[u, 1])
        put(A(lz, u, ms), A(loc, u, ms)[...] + val(A(lr, u, ms)) + val(A(lz, u, ms)))
        mid_sends["Ams"](u).start()

    def m_Bsm2(u):
        got(B(lr, u, sm), rrB.at[u])
        put(DB(u, sm), val(B(lz, u, sm)) + val(B(lr, u, sm)))
        mid_sends["Bsm2O"](u).start()
        mid_sends["Bsm2I"](u).start()

    def m_back(where, sem, k, names):
        def f(u):
            got(where(u, k), sem.at[u, k])
            for name in names:
                mid_sends[name](u).start()
        return f

    def m_fin(u):
        pl.semaphore_wait(free.at[u], 1)
        fin_copy(u, 1).start()
        for k in (ns, no):
            got(DA(u, k), bA.at[u, k])
        fin_copy(u, 0).start()

    end_events = dict(loc=ev_loc, lA=ev_lA(end_sends), lB=e_lB, Amo=e_Amo, Ams=e_Ams, Bse=e_Bse,
                      Bse2=e_Bse2, bAmo=e_bAmo, fin=e_fin)
    mid_events = dict(loc=ev_loc, lA=ev_lA(mid_sends), Bo=m_Bo, Amo=m_Amo, Bs=m_Bs, Ams=m_Ams, Bsm2=m_Bsm2,
                      bAms=m_back(DA, bA, ms, ("bAmsI", "bAmsR")), bAmo=m_back(DA, bA, mo, ("bAmoO", "bAmoR")),
                      bBse=m_back(DB, bB, se, ("bBse",)), bBom=m_back(DB, bB, om, ("bBom",)),
                      bBoe=m_back(DB, bB, oe, ("bBoe",)), fin=m_fin)

    def events(i, pos):
        for here, when, handlers in ((is_end, END, end_events), (is_mid, MID, mid_events)):
            @pl.when(here)
            def _():
                for name, off in sorted(when.items(), key=lambda kv: kv[1]):
                    if int(off) % 2 == pos:
                        u = i - int(off) // 2

                        @pl.when((u >= 0) & (u < UNITS))
                        def _():
                            handlers[name](u)

    def body(i, carry):
        t, h = i // 2, lax.rem(i, 2)

        @pl.when((i < UNITS) & (h == 0))
        def _():
            @pl.when(t + 1 < STAGES)
            def _():
                load(t + 1)

            hidden_part(t)

            @pl.when(t == 0)
            def _():
                weights[1].wait()
                weights[2].wait()

        for pos in range(2):
            @pl.when(i < UNITS)
            def _():
                term_part(t, 2 * h + pos)

            if pos == 1:
                @pl.when(i == UNITS - 1)
                def _():
                    load_x(0)

            @pl.when((i >= UNITS) & (i < UNITS + TILES))
            def _():
                grad_part(2 * (i - UNITS) + pos)

            events(i, pos)
        return carry

    weights[0].wait()
    lax.fori_loop(0, LOOPS, body, 0)

    def drain(u, carry):
        @pl.when(is_end)
        def _():
            for send in end_sends.values():
                send(u).wait_send()

        @pl.when(is_mid)
        def _():
            for send in mid_sends.values():
                send(u).wait_send()

        for k in range(2):
            fin_copy(u, k).wait_send()
            fin_wait(u, k)
        return carry

    lax.fori_loop(0, UNITS, drain, 0)
    for t in (STAGES - 2, STAGES - 1):
        for q in range(Q):
            sib_copy(t, q).wait_send()


def flush_kernel(*refs):
    sem = refs[-1]
    n = (len(refs) - 1) // 2
    copies = []
    for k in range(n):
        rows = refs[k].shape[0] // PARTS
        for p in range(PARTS):
            at = pl.ds(p * rows, rows)
            copies.append(pltpu.make_async_copy(refs[k].at[at], refs[n + k].at[at], sem.at[k, p]))
    for c in copies:
        c.start()
    for c in copies:
        c.wait()


def solution(mesh):
    dma = pltpu.SemaphoreType.DMA
    shapes = ((TOKENS, D), (D, HID), (D, HID), (HID, D))

    def step(x, dy, gate, up, w_gate, w_up, w_down):
        hbm = pl.BlockSpec(memory_space=pltpu.HBM)
        vmem = pl.BlockSpec(memory_space=pltpu.VMEM)
        held = pl.pallas_call(
            tree_kernel,
            out_shape=tuple(pltpu.VMEM(s, BF16) for s in shapes),
            in_specs=[hbm] * 7,
            out_specs=(vmem,) * 4,
            scratch_shapes=[
                pltpu.VMEM((2, 2 * ROWS, D), BF16),
                pltpu.VMEM((2, 2 * ROWS, HID), BF16), pltpu.VMEM((2, 2 * ROWS, HID), BF16),
                pltpu.VMEM((2, TOKENS, TILE), BF16),
                pltpu.VMEM((HALF, D), F32), pltpu.VMEM((2, ROWS, D), BF16),
                pltpu.VMEM((TOKENS, 2 * HID), BF16), pltpu.VMEM((TOKENS, HID), BF16),
                pltpu.VMEM((HALF, D), BF16), pltpu.VMEM((HALF, D), BF16),
                pltpu.VMEM((UNITS * BLOCK, WB), BF16),
                dma((3,)), dma((2, 6)), dma((2,)), pltpu.SemaphoreType.REGULAR((UNITS,)),
                dma((STAGES, Q)), dma((STAGES, Q)), dma((UNITS, 2)), dma((UNITS, 2)),
                dma((UNITS, 7)), dma((UNITS, 8)), dma((UNITS,)), dma((UNITS, 2)), dma((UNITS, 4)),
                dma((UNITS, 2)), dma((UNITS,)), dma((UNITS,)), dma((UNITS, 4)),
            ],
            compiler_params=pltpu.CompilerParams(
                collective_id=0, has_side_effects=True, vmem_limit_bytes=42 * 2**20),
        )(x, dy, gate, up, w_gate, w_up, w_down)
        return pl.pallas_call(
            flush_kernel,
            out_shape=tuple(jax.ShapeDtypeStruct(s, BF16) for s in shapes),
            in_specs=[vmem] * 4,
            out_specs=(hbm,) * 4,
            scratch_shapes=[dma((4, PARTS))],
            compiler_params=pltpu.CompilerParams(vmem_limit_bytes=2 * 2**20),
        )(*held)

    tokens, columns, rows = P("dp", None), P(None, "tp"), P("tp", None)
    return jax.shard_map(
        step,
        mesh=mesh,
        in_specs=(tokens, tokens, P("dp", "tp"), P("dp", "tp"), columns, columns, rows),
        out_specs=(tokens, P("dp", "tp"), P("dp", "tp"), P(("dp", "tp"), None)),
        check_vma=False,
    )
```
